128 devices in a mesh: ev: 8 (over z, core), mesh: 16 (over y, x).
Axes of the slice: x: 4, y: 4, z: 4, core: 2. Of those that a mesh axis runs over, the one named last changes fastest.
Arguments:
- kernels: bfloat16 [16, 12, 4096, 128], P('ev', None, 'mesh'), may hold values from -6 to 6
- tile_owner: int32 [16, 8192, 1], P('ev', 'mesh'), may hold values from 0 to 15; in each aligned block of 512 rows (0 to 511, 512 to 1023, ..., all dimensions but the last counted through in order) at most 64 rows name the same one
- tile_source: int32 [16, 8192], P('ev', 'mesh'), may hold values from 0 to 255
- tile_target: int32 [16, 8192], P('ev', 'mesh'), may hold values from 0 to 63
- tile_seed: int32 [16, 8192], P('ev', 'mesh'), may hold values from 0 to 83
- tile_count: int32 [16, 16], P('ev', 'mesh'), may hold values from 256 to 512
- prev_gradient: float32 [12, 16, 64, 128], P(None, 'mesh', 'ev'), may hold values from -18 to 18
- prev_step: float32 [12, 16, 64, 128], P(None, 'mesh', 'ev'), may hold values from -18 to 18, as said below
- precond: float32 [12, 16, 64, 128], P(None, 'mesh', 'ev'), may hold values from 0.2 to 2
Outputs:
- inversion_direction: float32 [12, 16, 64, 128], P(None, 'mesh', 'ev')
- event_direction: float32 [16, 12, 4096, 128], P('ev', None, 'mesh')
The draws below stay inside these ranges and needn't reach their ends.
Inputs may be any that keep to these rules, and one draw needn't show every extreme that they name: `tile_owner`: in every aligned block of 512 rows (one event's list for one partition) no partition is named by more than 64 rows, a bound that some block reaches. Rows of a list at positions tile_count or later are padding. prev_step = -c * prev_gradient cell by cell, with c between 0.1 and 1.
All inputs are finite; a program needn't handle non-finite values.
Results may differ from the reference program's by a relative error of at most 0.0003.
The reference program's roundings to bfloat16 on the way count: a program that leaves them out, or rounds other values in their place, can miss the bound.
Values may be sent and summed in bfloat16 or wider, within the bound.
A program may use at most 128 MiB of HBM per device.

```python
import math
import jax
import jax.numpy as jnp
import numpy as np
from jax import lax

C = 12
NODES = 128
EB_DEV = 256
TILES_DEV = 512
PARTITIONS = 16
EVENTS = 16
EBLOCKS = 4096
ISUB = 64
IBLOCKS = 1024
CAP = 64


def history_pair(key):
    base = jax.random.fold_in(key, 11)
    first, second = jax.random.split(base)
    shape = (C, PARTITIONS, ISUB, NODES)
    older = jnp.clip(3.0 * jax.random.normal(first, shape, jnp.float32), -18.0, 18.0)
    factor = jnp.exp(jax.random.uniform(second, shape, jnp.float32, math.log(0.1), 0.0))
    return (older, -factor * older)


def draw_prev_gradient(key, part):
    return history_pair(key)[0]


def draw_prev_step(key, part):
    return history_pair(key)[1]


def place_ends(values, own_key, low, largest):
    shape = values.shape
    place = [jax.random.randint(jax.random.fold_in(own_key, axis), (), 0, shape[axis]) for axis in range(len(shape))]
    values = values.at[tuple(place)].set(low)
    longest = shape.index(max(shape))
    place[longest] = (place[longest] + 1) % shape[longest]
    return values.at[tuple(place)].set(largest)


def block_levels(stream_key, extent, shards, low, top_value):
    def one(dim, blocks):
        heights = jax.random.uniform(jax.random.fold_in(jax.random.fold_in(stream_key, 6), dim), (blocks,), jnp.float32, low / len(shards), top_value / len(shards))
        return jnp.repeat(jnp.exp(heights), extent[dim] // blocks).reshape((-1,) + (1,) * (len(extent) - dim - 1))

    gain = one(*shards[0])
    for cut in shards[1:]:
        gain = gain * one(*cut)
    return gain


def routed_block(rng, own, number, rows, count, top, most, lean):
    sequence = jax.random.permutation(rng, count)
    heavy_load, common = shares(count, rows * top, most, lean, True), shares(count, rows * top, most, lean, False)
    places = jnp.arange(count)

    def named(tallies, rotation):
        used = int((tallies > 0).sum())
        fixed = max(1, used // 4)
        passed = fixed + (places - fixed + rotation * (used - fixed)) % max(1, count - fixed)
        return jnp.zeros((count,), jnp.int32).at[sequence[jnp.where(places < fixed, places, passed)]].set(jnp.asarray(tallies, jnp.int32))

    tallies = jnp.where(number % 4 == 0, named(heavy_load, number // 4), named(common, number - number // 4 - 1))
    mixed = jax.random.permutation(jax.random.fold_in(own, 3), count)
    source_of, taker = mixed[0:count // 2 * 2:2], mixed[1:count // 2 * 2:2]
    margin = jnp.minimum(tallies[source_of] - 1, most - tallies[taker]) // 2
    margin = jnp.where((source_of == sequence[0]) | (taker == sequence[0]) | (tallies[taker] == 0), 0, jnp.maximum(margin, 0))
    passed = jax.random.randint(jax.random.fold_in(own, 4), (count // 2,), 0, 1 << 20) % (margin + 1)
    tallies = tallies.at[source_of].add(-passed).at[taker].add(passed)
    items = jnp.searchsorted(jnp.cumsum(tallies), jnp.arange(rows * top), side="right").astype(jnp.int32)
    listing = items.reshape(top, rows).T
    listing = listing[jax.random.permutation(jax.random.fold_in(own, 1), rows)]
    rotation = jax.random.randint(jax.random.fold_in(own, 2), (rows, 1), 0, top)
    return jnp.take_along_axis(listing, (jnp.arange(top)[None, :] + rotation) % top, axis=1)


def shares(number_of, total, most, slope, full):
    weights = [(1 << 20) // math.isqrt(rank ** slope) + 1 for rank in range(1, number_of + 1)]
    largest = most if full else min(most, max(-(-total // number_of), total * weights[0] // sum(weights)))
    least = 1 if total - largest >= number_of - 1 else 0
    counts, surplus = [largest] + [least] * (number_of - 1), total - largest - least * (number_of - 1)
    while surplus > 0:
        free = [i for i in range(1, number_of) if counts[i] < largest] or [i for i in range(1, number_of) if counts[i] < most]
        pool, left = sum([weights[i] for i in free]), surplus
        for i in free:
            addition = min(most - counts[i], max(1, left * weights[i] // pool), surplus)
            counts[i] = counts[i] + addition
            surplus = surplus - addition
    return np.array(counts)


def bell_draw(key, extent, deviation, most, cuts=(), kind=jnp.bfloat16):
    values = jax.random.normal(key, extent, jnp.float32) * deviation
    if len(cuts) > 0:
        values = block_levels(key, extent, cuts, -0.22, 0.18) * values
    return jnp.clip(values, min=-most, max=most).astype(kind)


def setup_inputs(seed: int = 0) -> dict:
    keys = jax.random.split(jax.random.key(seed), 10)
    kernels = bell_draw(keys[0], (EVENTS, C, EBLOCKS, NODES), 1.0, 6.0, ((0, 8), (2, 16)))
    tile_owner_keys = jax.random.split(jax.random.fold_in(keys[1], 1), EVENTS * (PARTITIONS * TILES_DEV) // TILES_DEV)
    tile_owner_turns = jax.random.permutation(jax.random.fold_in(keys[1], 3), EVENTS * (PARTITIONS * TILES_DEV) // TILES_DEV)
    tile_owner = jax.vmap(lambda own, number: routed_block(jax.random.fold_in(keys[1], 2), own, number, TILES_DEV, PARTITIONS, 1, CAP, 2))(tile_owner_keys, tile_owner_turns).reshape((EVENTS, PARTITIONS * TILES_DEV, 1))
    tile_source = place_ends(jax.random.randint(keys[2], (EVENTS, PARTITIONS * TILES_DEV), 0, EB_DEV), jax.random.fold_in(keys[2], 1), 0, EB_DEV - 1).astype(jnp.int32)
    tile_target = place_ends(jax.random.randint(keys[3], (EVENTS, PARTITIONS * TILES_DEV), 0, ISUB), jax.random.fold_in(keys[3], 1), 0, ISUB - 1).astype(jnp.int32)
    tile_seed = place_ends(jax.random.randint(keys[4], (EVENTS, PARTITIONS * TILES_DEV), 0, 84), jax.random.fold_in(keys[4], 1), 0, 83).astype(jnp.int32)
    tile_count = place_ends(jax.random.randint(keys[5], (EVENTS, PARTITIONS), TILES_DEV // 2, TILES_DEV + 1), jax.random.fold_in(keys[5], 1), TILES_DEV // 2, TILES_DEV).astype(jnp.int32)
    prev_gradient = draw_prev_gradient(jax.random.fold_in(keys[9], 71), 0)
    prev_step = draw_prev_step(jax.random.fold_in(keys[9], 71), 0)
    precond = jnp.clip(jnp.exp(math.log(2.0) - 2.3025851 * jax.random.uniform(keys[8], (C, PARTITIONS, ISUB, NODES), jnp.float32) ** block_levels(keys[8], (C, PARTITIONS, ISUB, NODES), ((1, 16), (2, 8)), -0.2, 0.2)), 0.2, 2.0)
    return dict(kernels=kernels, tile_owner=tile_owner, tile_source=tile_source, tile_target=tile_target, tile_seed=tile_seed, tile_count=tile_count, prev_gradient=prev_gradient, prev_step=prev_step, precond=precond)


def make_tiles(seed_ids):
    node_pos = jnp.arange(NODES).astype(jnp.float32)
    seed_ids = seed_ids.astype(jnp.int32)
    offset = (seed_ids % 7 - 3).astype(jnp.float32)
    spread = 0.55 + 0.1 * ((seed_ids // 7) % 3).astype(jnp.float32)
    weight = 0.1 + 0.1 * (seed_ids // 21).astype(jnp.float32)
    distance = node_pos[None, :, None] - node_pos[None, None, :] - offset[:, None, None]
    values = weight[:, None, None] * jnp.exp(-distance * distance / (2.0 * spread * spread)[:, None, None])
    return values.astype(jnp.bfloat16)


def reference(kernels, tile_owner, tile_source, tile_target, tile_seed, tile_count, prev_gradient, prev_step, precond):
    groups = EVENTS * PARTITIONS
    owner_ids = tile_owner.reshape(groups, TILES_DEV).astype(jnp.int32)
    source_ids = tile_source.reshape(groups, TILES_DEV).astype(jnp.int32)
    target_ids = tile_target.reshape(groups, TILES_DEV).astype(jnp.int32)
    seed_ids = tile_seed.reshape(groups, TILES_DEV).astype(jnp.int32)
    limits = tile_count.reshape(groups).astype(jnp.int32)
    group_ids = jnp.arange(groups, dtype=jnp.int32)
    group_event = group_ids // PARTITIONS
    group_part = group_ids % PARTITIONS
    position = jnp.arange(TILES_DEV, dtype=jnp.int32)

    def forward(total, inputs):
        owners, sources, targets, seeds, event, part, limit = inputs
        field = lax.dynamic_index_in_dim(kernels, event, 0, keepdims=False)
        picked = jnp.transpose(field[:, part * EB_DEV + sources, :], (1, 0, 2))
        tile_mats = make_tiles(seeds)
        product = jnp.einsum('tcn,tnm->tcm', picked.astype(jnp.float32), tile_mats.astype(jnp.float32))
        live_mask = (position < limit).astype(jnp.float32)
        contribution = (product * live_mask[:, None, None]).astype(jnp.bfloat16)
        blocks = owners * ISUB + targets
        added = jax.ops.segment_sum(contribution.astype(jnp.float32), blocks, num_segments=IBLOCKS)
        return total + added, None

    start = jnp.zeros((IBLOCKS, C, NODES), jnp.float32)
    summed, _ = lax.scan(forward, start, (owner_ids, source_ids, target_ids, seed_ids, group_event, group_part, limits))
    gradient = jnp.transpose(summed.reshape(PARTITIONS, ISUB, C, NODES), (2, 0, 1, 3))

    change = gradient - prev_gradient
    curvature = jnp.sum(prev_step * change)
    alpha = jnp.sum(prev_step * gradient) / curvature
    scaled = precond * (gradient - alpha * change)
    beta = jnp.sum(change * scaled) / curvature
    inversion_direction = -(scaled + (alpha - beta) * prev_step)

    rounded = inversion_direction.astype(jnp.bfloat16)
    flat_direction = jnp.transpose(rounded.reshape(C, IBLOCKS, NODES), (1, 0, 2))

    def per_event(event):
        def backward(total, part):
            group = event * PARTITIONS + part
            owners = lax.dynamic_index_in_dim(owner_ids, group, 0, keepdims=False)
            sources = lax.dynamic_index_in_dim(source_ids, group, 0, keepdims=False)
            targets = lax.dynamic_index_in_dim(target_ids, group, 0, keepdims=False)
            seeds = lax.dynamic_index_in_dim(seed_ids, group, 0, keepdims=False)
            limit = lax.dynamic_index_in_dim(limits, group, 0, keepdims=False)
            picked = flat_direction[owners * ISUB + targets]
            tile_mats = make_tiles(seeds)
            product = jnp.einsum('tcm,tnm->tcn', picked.astype(jnp.float32), tile_mats.astype(jnp.float32))
            live_mask = (position < limit).astype(jnp.float32)
            product = product * live_mask[:, None, None]
            added = jax.ops.segment_sum(product, part * EB_DEV + sources, num_segments=EBLOCKS)
            return total + added, None

        empty = jnp.zeros((EBLOCKS, C, NODES), jnp.float32)
        result, _ = lax.scan(backward, empty, jnp.arange(PARTITIONS, dtype=jnp.int32))
        return jnp.transpose(result, (1, 0, 2))

    event_direction = lax.map(per_event, jnp.arange(EVENTS, dtype=jnp.int32))
    return inversion_direction, event_direction
```

```python
import functools, math
import jax, jax.numpy as jnp
from jax import lax
from jax.experimental import pallas as pl
from jax.experimental.pallas import tpu as pltpu
from jax.sharding import PartitionSpec as P

C=12; N=128; E=256; T=512; V=2; S=84

def fill_tables(ext, table, flip):
    i = lax.broadcasted_iota(jnp.int32,(136,N),0).astype(jnp.float32) - 4.0
    j = lax.broadcasted_iota(jnp.int32,(136,N),1).astype(jnp.float32)
    d = i - j
    for sp in range(3):
        spread = jnp.float32(0.55) + jnp.float32(0.1)*jnp.float32(sp)
        e = jnp.exp(-d*d/(jnp.float32(2.0)*spread*spread))
        for wt in range(4):
            weight = jnp.float32(0.1)+jnp.float32(0.1)*jnp.float32(wt)
            ext[wt*3+sp] = weight*e
    for k in range(12):
        for o in range(7):
            off = o-3
            if flip: off = -off
            table[k*7+o] = ext[k, pl.ds(4-off,N),:].astype(jnp.bfloat16)

def fwd_kernel(code, k_ref, out_ref, ext, table, xs, scr):
    fill_tables(ext, table, False)
    for v in range(V):
        @pl.loop(0, E//16)
        def _(b):
            e0 = pl.multiple_of(b*16,16)
            for c in range(C):
                x = k_ref[v, c, pl.ds(e0,16), :].astype(jnp.float32)
                xs[pl.ds((v*E+e0)*C+c, 16, stride=C), :] = x
    U=16
    @pl.loop(0, V*T//U)
    def _(g):
        t0 = g*U
        for u in range(U):
            w = code[t0+u]
            seed = w & 127
            src = (w >> 7) & 511
            x = xs[pl.ds(src*C,16),:].astype(jnp.bfloat16)
            y = jnp.dot(x, table[seed], preferred_element_type=jnp.float32)
            scr[pl.ds(u*16,16),:] = y
        r0 = pl.multiple_of(t0,16)
        for c in range(C):
            out_ref[pl.ds(r0,U), c*N:(c+1)*N] = scr[pl.ds(c,U,stride=16),:].astype(jnp.bfloat16)

def forward(code, kern, cost=None):
    return pl.pallas_call(fwd_kernel,
        out_shape=jax.ShapeDtypeStruct((V*T, C*N), jnp.bfloat16),
        grid_spec=pltpu.PrefetchScalarGridSpec(num_scalar_prefetch=1, grid=(),
            in_specs=[pl.BlockSpec(memory_space=pltpu.VMEM)],
            out_specs=pl.BlockSpec(memory_space=pltpu.VMEM),
            scratch_shapes=[pltpu.VMEM((12,136,N),jnp.float32), pltpu.VMEM((S,N,N),jnp.bfloat16),
                pltpu.VMEM((V*E*C+16,N),jnp.float32), pltpu.VMEM((16*16,N),jnp.float32)]),
        compiler_params=pltpu.CompilerParams(vmem_limit_bytes=48<<20),
        name="fwd")(code, kern)

def bwd_kernel(code, d_ref, out_ref, ext, table, xs, acc0, acc1):
    fill_tables(ext, table, True)
    @pl.loop(0, 128)
    def _(b):
        xs[pl.ds(pl.multiple_of(b*96,96),96),:] = d_ref[b].astype(jnp.float32)
    zero = jnp.zeros((64,N),jnp.float32)
    @pl.loop(0, (E*C)//64)
    def _(b):
        acc0[pl.ds(pl.multiple_of(b*64,64),64),:] = zero
        acc1[pl.ds(pl.multiple_of(b*64,64),64),:] = zero
    U=8
    @pl.loop(0, T//U)
    def _(g):
        for u in range(U):
            for v in range(V):
                w = code[v*T+g*U+u]
                seed = w & 127
                dst = jnp.minimum(w >> 16, 1023)
                src = (w >> 7) & 255
                row = jnp.where((w >> 16) >= 1024, E*C, src*C)
                x = xs[pl.ds(dst*C,16),:].astype(jnp.bfloat16)
                y = jnp.dot(x, table[seed], preferred_element_type=jnp.float32)
                acc = (acc0,acc1)[v]
                acc[pl.ds(row,8),:] += y[:8]
                acc[pl.ds(row+8,4),:] += y[8:12]
    for v in range(V):
        acc = (acc0,acc1)[v]
        @pl.loop(0, E//8)
        def _(b):
            e0 = pl.multiple_of(b*8,8)
            for c in range(C):
                out_ref[v, c, pl.ds(e0,8), :] = acc[pl.ds(e0*C+c, 8, stride=C),:]

def backward(code, dirs):
    return pl.pallas_call(bwd_kernel,
        out_shape=jax.ShapeDtypeStruct((V, C, E, N), jnp.float32),
        grid_spec=pltpu.PrefetchScalarGridSpec(num_scalar_prefetch=1, grid=(),
            in_specs=[pl.BlockSpec(memory_space=pltpu.VMEM)],
            out_specs=pl.BlockSpec(memory_space=pltpu.VMEM),
            scratch_shapes=[pltpu.VMEM((12,136,N),jnp.float32), pltpu.VMEM((S,N,N),jnp.bfloat16),
                pltpu.VMEM((1024*C+16,N),jnp.float32), pltpu.VMEM((E*C+16,N),jnp.float32), pltpu.VMEM((E*C+16,N),jnp.float32)]),
        compiler_params=pltpu.CompilerParams(vmem_limit_bytes=48<<20),
        name="bwd")(code, dirs)


def body(kernels, tile_owner, tile_source, tile_target, tile_seed, tile_count, prev_gradient, prev_step, precond):
    pos = lax.broadcasted_iota(jnp.int32, (V, T), 1)
    live = pos < tile_count
    block = tile_owner.reshape(V, T) * 64 + tile_target
    src = tile_source + E * lax.broadcasted_iota(jnp.int32, (V, T), 0)
    block = jnp.where(live, block, 1024)
    code = (tile_seed + (src << 7) + (block << 16)).reshape(V * T)
    contribution = forward(code, kernels)
    hits = (jnp.arange(1024, dtype=jnp.int32)[:, None] == block.reshape(1, V * T)).astype(jnp.bfloat16)
    partial = jnp.dot(hits, contribution, preferred_element_type=jnp.float32)
    owned = lax.psum_scatter(partial, ("mesh", "ev"), scatter_dimension=0, tiled=True)
    gradient = jnp.transpose(owned.reshape(8, C, N), (1, 0, 2))[:, None]
    change = gradient - prev_gradient
    weighted = precond * change
    sums = jnp.stack([jnp.sum(prev_step * change), jnp.sum(prev_step * gradient), jnp.sum(weighted * gradient), jnp.sum(weighted * change)])
    curvature, slope, cross_term, self_term = lax.psum(sums, ("mesh", "ev"))
    alpha = slope / curvature
    scaled = precond * (gradient - alpha * change)
    beta = (cross_term - alpha * self_term) / curvature
    direction = -(scaled + (alpha - beta) * prev_step)
    local = jnp.transpose(direction.astype(jnp.bfloat16)[:, 0], (1, 0, 2)).reshape(1, 8 * C, N)
    dirs = lax.all_gather(local, ("mesh", "ev"), axis=0, tiled=True)
    return direction, backward(code, dirs)


def solution(mesh):
    in_specs = (
        P("ev", None, "mesh", None),
        P("ev", "mesh", None),
        P("ev", "mesh"),
        P("ev", "mesh"),
        P("ev", "mesh"),
        P("ev", "mesh"),
        P(None, "mesh", "ev", None),
        P(None, "mesh", "ev", None),
        P(None, "mesh", "ev", None),
    )
    out_specs = (P(None, "mesh", "ev", None), P("ev", None, "mesh", None))
    return jax.shard_map(body, mesh=mesh, in_specs=in_specs, out_specs=out_specs, check_vma=False)
```

```python
import functools, math
import jax, jax.numpy as jnp
from jax import lax
from jax.experimental import pallas as pl
from jax.experimental.pallas import tpu as pltpu
from jax.sharding import PartitionSpec as P

C=12; N=128; E=256; T=512; V=2; S=84

def fill_tables(ext, table, flip):
    i = lax.broadcasted_iota(jnp.int32,(136,N),0).astype(jnp.float32) - 4.0
    j = lax.broadcasted_iota(jnp.int32,(136,N),1).astype(jnp.float32)
    d = i - j
    for sp in range(3):
        spread = jnp.float32(0.55) + jnp.float32(0.1)*jnp.float32(sp)
        e = jnp.exp(-d*d/(jnp.float32(2.0)*spread*spread))
        for wt in range(4):
            weight = jnp.float32(0.1)+jnp.float32(0.1)*jnp.float32(wt)
            ext[wt*3+sp] = weight*e
    for k in range(12):
        for o in range(7):
            off = o-3
            if flip: off = -off
            table[k*7+o] = ext[k, pl.ds(4-off,N),:].astype(jnp.bfloat16)

def fwd_kernel(code, k_ref, out_ref, ext, table, xs, scr):
    fill_tables(ext, table, False)
    for v in range(V):
        @pl.loop(0, E//16)
        def _(b):
            e0 = pl.multiple_of(b*16,16)
            for c in range(C):
                x = k_ref[v, c, pl.ds(e0,16), :].astype(jnp.float32)
                xs[pl.ds((v*E+e0)*C+c, 16, stride=C), :] = x
    U=16
    @pl.loop(0, V*T//U)
    def _(g):
        t0 = g*U
        for u in range(U):
            w = code[t0+u]
            seed = w & 127
            src = (w >> 7) & 511
            x = xs[pl.ds(src*C,16),:].astype(jnp.bfloat16)
            y = jnp.dot(x, table[seed], preferred_element_type=jnp.float32)
            scr[pl.ds(u*16,16),:] = y
        r0 = pl.multiple_of(t0,16)
        for c in range(C):
            out_ref[pl.ds(r0,U), c*N:(c+1)*N] = scr[pl.ds(c,U,stride=16),:].astype(jnp.bfloat16)

def forward(code, kern, cost=None):
    return pl.pallas_call(fwd_kernel,
        out_shape=jax.ShapeDtypeStruct((V*T, C*N), jnp.bfloat16),
        grid_spec=pltpu.PrefetchScalarGridSpec(num_scalar_prefetch=1, grid=(),
            in_specs=[pl.BlockSpec(memory_space=pltpu.VMEM)],
            out_specs=pl.BlockSpec(memory_space=pltpu.VMEM),
            scratch_shapes=[pltpu.VMEM((12,136,N),jnp.float32), pltpu.VMEM((S,N,N),jnp.bfloat16),
                pltpu.VMEM((V*E*C+16,N),jnp.float32), pltpu.VMEM((16*16,N),jnp.float32)]),
        compiler_params=pltpu.CompilerParams(vmem_limit_bytes=48<<20),
        name="fwd")(code, kern)

def bwd_kernel(code, d_ref, out_ref, ext, table, xs, acc0, acc1):
    fill_tables(ext, table, True)
    for k in range(3):
        a1, a2, a3 = AXES[k]
        for rc in range(2):
            @pl.loop(0, 64)
            def _(b):
                r = b >> 4
                q = b & 15
                base = r*WEIGHT[a1] + (q >> 2)*WEIGHT[a2] + (q & 3)*WEIGHT[a3] + rc*8
                piece = d_ref[k, rc, r, q].astype(jnp.float32)
                for cc in range(4):
                    xs[pl.ds(base*C + k*4 + cc, 8, stride=C), :] = piece[cc*8:cc*8+8]
    zero = jnp.zeros((64,N),jnp.float32)
    @pl.loop(0, (E*C)//64)
    def _(b):
        acc0[pl.ds(pl.multiple_of(b*64,64),64),:] = zero
        acc1[pl.ds(pl.multiple_of(b*64,64),64),:] = zero
    U=8
    @pl.loop(0, T//U)
    def _(g):
        for u in range(U):
            for v in range(V):
                w = code[v*T+g*U+u]
                seed = w & 127
                dst = jnp.minimum(w >> 16, 1023)
                src = (w >> 7) & 255
                row = jnp.where((w >> 16) >= 1024, E*C, src*C)
                x = xs[pl.ds(dst*C,16),:].astype(jnp.bfloat16)
                y = jnp.dot(x, table[seed], preferred_element_type=jnp.float32)
                acc = (acc0,acc1)[v]
                acc[pl.ds(row,8),:] += y[:8]
                acc[pl.ds(row+8,4),:] += y[8:12]
    for v in range(V):
        acc = (acc0,acc1)[v]
        @pl.loop(0, E//8)
        def _(b):
            e0 = pl.multiple_of(b*8,8)
            for c in range(C):
                out_ref[v, c, pl.ds(e0,8), :] = acc[pl.ds(e0*C+c, 8, stride=C),:]

def backward(code, dirs):
    return pl.pallas_call(bwd_kernel,
        out_shape=jax.ShapeDtypeStruct((V, C, E, N), jnp.float32),
        grid_spec=pltpu.PrefetchScalarGridSpec(num_scalar_prefetch=1, grid=(),
            in_specs=[pl.BlockSpec(memory_space=pltpu.VMEM)],
            out_specs=pl.BlockSpec(memory_space=pltpu.VMEM),
            scratch_shapes=[pltpu.VMEM((12,136,N),jnp.float32), pltpu.VMEM((S,N,N),jnp.bfloat16),
                pltpu.VMEM((1024*C+16,N),jnp.float32), pltpu.VMEM((E*C+16,N),jnp.float32), pltpu.VMEM((E*C+16,N),jnp.float32)]),
        compiler_params=pltpu.CompilerParams(vmem_limit_bytes=48<<20),
        name="bwd")(code, dirs)


AXES = ((0, 1, 2), (1, 2, 0), (2, 0, 1))
WEIGHT = (256, 64, 16)
MESH_ID = pl.DeviceIdType.MESH


def comm_kernel(code_ref, con_ref, pg_ref, ps_ref, pc_ref, dir_ref, tab_ref,
                give, take, own, s1, s2, pr, row, rows,
                gs, gr, s1s, s1r, s2s, s2r, ps, pr_sem, rs, rr, aps, apr, ars, arr, a2s, a2r, ads, adr):
    e = lax.axis_index("ev")
    m = lax.axis_index("mesh")
    me = e * 16 + m
    at = (lax.rem(m, 4), lax.div(m, 4), lax.div(e, 2))
    core = lax.rem(e, 2)

    def place(k, r, i, j, other=False):
        off = [0, 0, 0]
        for axis, o in zip(AXES[k], (r, i, j)):
            off[axis] = o % 4
        x, y, z = (lax.rem(a + o, 4) if o else a for a, o in zip(at, off))
        return {"ev": z * 2 + (1 - core if other else core), "mesh": y * 4 + x}

    def send(src, dst, ssem, rsem, where):
        copy = pltpu.make_async_remote_copy(src_ref=src, dst_ref=dst, send_sem=ssem, recv_sem=rsem,
                                            device_id=where, device_id_type=MESH_ID)
        copy.start()

    def got(ref, ssem, rsem):
        pltpu.make_async_remote_copy(src_ref=ref, dst_ref=ref, send_sem=ssem, recv_sem=rsem,
                                     device_id=place(0, 0, 0, 0, True), device_id_type=MESH_ID).wait_recv()

    def sent(ref, ssem, rsem):
        pltpu.make_async_remote_copy(src_ref=ref, dst_ref=ref, send_sem=ssem, recv_sem=rsem,
                                     device_id=place(0, 0, 0, 0, True), device_id_type=MESH_ID).wait_send()

    barrier = pltpu.get_barrier_semaphore()

    def greet(d, carry):
        other = lax.rem(me + d, 128)
        pl.semaphore_signal(barrier, inc=1, device_id={"ev": lax.div(other, 16), "mesh": lax.rem(other, 16)},
                            device_id_type=MESH_ID)
        return carry

    lax.fori_loop(1, 128, greet, 0)

    ids = lax.broadcasted_iota(jnp.int32, (128, N), 0)
    i_of, j_of, sub = ids >> 5, (ids >> 3) & 3, ids & 7
    block = code_ref[...] >> 16

    def partial(k, r, other):
        a1, a2, a3 = AXES[k]
        rows_k = i_of * WEIGHT[a2] + j_of * WEIGHT[a3] + sub
        wanted = block - (r * WEIGHT[a1] + (8 if other else 0))
        hits = jnp.concatenate([(rows_k == wanted[:, l * N:(l + 1) * N]).astype(jnp.float32).astype(jnp.bfloat16) for l in range(8)], axis=1)
        return jnp.dot(hits, con_ref[:, k * 512:(k + 1) * 512], preferred_element_type=jnp.float32)

    order = (2, 1, 3, 0)
    for r in order:
        for k in range(3):
            got_k = partial(k, r, True)
            for cc in range(4):
                give[k, r, :, cc * 8:cc * 8 + 8, :] = got_k[:, cc * N:(cc + 1) * N].reshape(16, 8, N)
            if r == 2 and k == 0:
                pl.semaphore_wait(barrier, 127)
            send(give.at[k, r], take.at[k, r], gs.at[k, r], gr.at[k, r], place(0, 0, 0, 0, True))
    for r in order:
        for k in range(3):
            mine = partial(k, r, False)
            got(take.at[k, r], gs.at[k, r], gr.at[k, r])
            for cc in range(4):
                own[k, r, :, cc * 8:cc * 8 + 8, :] = mine[:, cc * N:(cc + 1) * N].reshape(16, 8, N) + take[k, r, :, cc * 8:cc * 8 + 8, :]
            up, down = place(k, 1, 0, 0), place(k, 3, 0, 0)
            if r == 2:
                send(own.at[k, 2, pl.ds(0, 8)], s1.at[k, 0], s1s.at[k, 0], s1r.at[k, 0], up)
                send(own.at[k, 2, pl.ds(8, 8)], s1.at[k, 1], s1s.at[k, 1], s1r.at[k, 1], down)
            if r == 1:
                send(own.at[k, 1, pl.ds(8, 8)], s2.at[k, 0, pl.ds(8, 8)], s2s.at[k, 0, 1], s2r.at[k, 0, 1], up)
            if r == 3:
                send(own.at[k, 3, pl.ds(0, 8)], s2.at[k, 1, pl.ds(0, 8)], s2s.at[k, 1, 0], s2r.at[k, 1, 0], down)
    for k in range(3):
        up, down = place(k, 1, 0, 0), place(k, 3, 0, 0)
        got(s1.at[k, 0], s1s.at[k, 0], s1r.at[k, 0])
        own[k, 1, 0:8] = own[k, 1, 0:8] + s1[k, 0]
        send(own.at[k, 1, pl.ds(0, 8)], s2.at[k, 0, pl.ds(0, 8)], s2s.at[k, 0, 0], s2r.at[k, 0, 0], up)
        got(s1.at[k, 1], s1s.at[k, 1], s1r.at[k, 1])
        own[k, 3, 8:16] = own[k, 3, 8:16] + s1[k, 1]
        send(own.at[k, 3, pl.ds(8, 8)], s2.at[k, 1, pl.ds(8, 8)], s2s.at[k, 1, 1], s2r.at[k, 1, 1], down)
    for k in range(3):
        for way in range(2):
            for half in range(2):
                got(s2.at[k, way, pl.ds(half * 8, 8)], s2s.at[k, way, half], s2r.at[k, way, half])
        own[k, 0] = own[k, 0] + s2[k, 0] + s2[k, 1]
        for q in range(1, 16):
            send(own.at[k, 0, q], pr.at[k, q - 1], ps.at[k], pr_sem.at[k], place(k, 0, q // 4, q % 4))
    parts = []
    for k in range(3):
        got(pr.at[k], ps.at[k], pr_sem.at[k])
        total = own[k, 0, 0]
        for q in range(15):
            total = total + pr[k, q]
        parts.append(total)
    gradient = jnp.concatenate(parts, axis=0)
    prev_g = pg_ref[...].reshape(96, N)
    step = ps_ref[...].reshape(96, N)
    cond = pc_ref[...].reshape(96, N)
    change = gradient - prev_g
    weighted = cond * change
    lane = lax.broadcasted_iota(jnp.int32, (1, N), 1)

    def summed(v):
        v = jnp.sum(v.reshape(12, 8, N), axis=0)
        return jnp.sum(jnp.sum(v, axis=0, keepdims=True), axis=1, keepdims=True)

    mine = jnp.zeros((1, N), jnp.float32)
    for n, v in enumerate((step * change, step * gradient, weighted * gradient, weighted * change)):
        mine = jnp.where(lane == n, summed(v), mine)
    row[...] = mine
    rows[me] = mine

    def tell(d, carry):
        other = lax.rem(me + d, 128)
        send(row, rows.at[me], rs, rr, {"ev": lax.div(other, 16), "mesh": lax.rem(other, 16)})
        return carry

    lax.fori_loop(1, 128, tell, 0)
    got(rows.at[pl.ds(0, 127)], rs, rr)
    totals = jnp.sum(rows[...], axis=0)
    curvature, slope, cross, self_ = (
        jnp.sum(jnp.where(lane == n, totals, 0.0), axis=1, keepdims=True) for n in range(4))
    alpha = slope / curvature
    beta = (cross - alpha * self_) / curvature
    scaled = cond * (gradient - alpha * change)
    direction = -(scaled + (alpha - beta) * step)
    dir_ref[...] = direction.reshape(12, 1, 8, N)
    rounded = direction.astype(jnp.bfloat16)
    partner = place(0, 0, 0, 0, True)
    for k in range(3):
        tab_ref[k, 0, 0, 0] = rounded[k * 32:(k + 1) * 32]
    for k in range(3):
        for q in range(1, 16):
            i, j = q // 4, q % 4
            back = (-i % 4) * 4 + (-j % 4)
            send(tab_ref.at[k, 0, 0, 0], tab_ref.at[k, 0, 0, back], aps.at[k], apr.at[k], place(k, 0, i, j))
    for k in range(3):
        got(tab_ref.at[k, 0, 0, pl.ds(1, 15)], aps.at[k], apr.at[k])
        send(tab_ref.at[k, 0, 0], tab_ref.at[k, 0, 3], ars.at[k, 0], arr.at[k, 0], place(k, 1, 0, 0))
        send(tab_ref.at[k, 0, 0], tab_ref.at[k, 0, 1], ars.at[k, 1], arr.at[k, 1], place(k, 3, 0, 0))
        send(tab_ref.at[k, 0, 0], tab_ref.at[k, 1, 0], ads.at[k, 0], adr.at[k, 0], partner)
    for k in range(3):
        got(tab_ref.at[k, 0, 3], ars.at[k, 0], arr.at[k, 0])
        send(tab_ref.at[k, 0, 3, pl.ds(0, 8)], tab_ref.at[k, 0, 2, pl.ds(0, 8)], a2s.at[k, 0], a2r.at[k, 0], place(k, 1, 0, 0))
        send(tab_ref.at[k, 0, 3], tab_ref.at[k, 1, 3], ads.at[k, 3], adr.at[k, 3], partner)
        got(tab_ref.at[k, 0, 1], ars.at[k, 1], arr.at[k, 1])
        send(tab_ref.at[k, 0, 1, pl.ds(8, 8)], tab_ref.at[k, 0, 2, pl.ds(8, 8)], a2s.at[k, 1], a2r.at[k, 1], place(k, 3, 0, 0))
        send(tab_ref.at[k, 0, 1], tab_ref.at[k, 1, 1], ads.at[k, 1], adr.at[k, 1], partner)
    for k in range(3):
        got(tab_ref.at[k, 0, 2, pl.ds(0, 8)], a2s.at[k, 0], a2r.at[k, 0])
        got(tab_ref.at[k, 0, 2, pl.ds(8, 8)], a2s.at[k, 1], a2r.at[k, 1])
        send(tab_ref.at[k, 0, 2], tab_ref.at[k, 1, 2], ads.at[k, 2], adr.at[k, 2], partner)
    for k in range(3):
        for r in range(4):
            got(tab_ref.at[k, 1, r], ads.at[k, r], adr.at[k, r])
    for k in range(3):
        for r in range(4):
            sent(give.at[k, r], gs.at[k, r], gr.at[k, r])
            sent(tab_ref.at[k, 0, r], ads.at[k, r], adr.at[k, r])
        for way in range(2):
            sent(s1.at[k, way], s1s.at[k, way], s1r.at[k, way])
            for half in range(2):
                sent(s2.at[k, way, pl.ds(half * 8, 8)], s2s.at[k, way, half], s2r.at[k, way, half])
            sent(tab_ref.at[k, 0, 0], ars.at[k, way], arr.at[k, way])
            sent(tab_ref.at[k, 0, 0, pl.ds(0, 8)], a2s.at[k, way], a2r.at[k, way])
        sent(pr.at[k], ps.at[k], pr_sem.at[k])
        sent(tab_ref.at[k, 0, 0, pl.ds(1, 15)], aps.at[k], apr.at[k])
    sent(rows.at[pl.ds(0, 127)], rs, rr)


def exchange(code, contribution, prev_gradient, prev_step, precond):
    dma = pltpu.SemaphoreType.DMA
    f32 = jnp.float32
    pairs = [dma((3, 4)), dma((3, 2)), dma((3, 2, 2)), dma((3,)), dma, dma((3,)), dma((3, 2)), dma((3, 2)), dma((3, 4))]
    return pl.pallas_call(
        comm_kernel,
        out_shape=(jax.ShapeDtypeStruct((C, 1, 8, N), f32), jax.ShapeDtypeStruct((3, 2, 4, 16, 32, N), jnp.bfloat16)),
        in_specs=[pl.BlockSpec(memory_space=pltpu.VMEM)] * 5,
        out_specs=(pl.BlockSpec(memory_space=pltpu.VMEM), pl.BlockSpec(memory_space=pltpu.VMEM)),
        scratch_shapes=[
            pltpu.VMEM((3, 4, 16, 32, N), f32), pltpu.VMEM((3, 4, 16, 32, N), f32), pltpu.VMEM((3, 4, 16, 32, N), f32),
            pltpu.VMEM((3, 2, 8, 32, N), f32), pltpu.VMEM((3, 2, 16, 32, N), f32), pltpu.VMEM((3, 15, 32, N), f32),
            pltpu.VMEM((1, N), f32), pltpu.VMEM((128, 1, N), f32),
        ] + [p for p in pairs for _ in range(2)],
        compiler_params=pltpu.CompilerParams(vmem_limit_bytes=48 << 20, collective_id=0, has_side_effects=True),
        name="exchange",
    )(code, contribution, prev_gradient, prev_step, precond)


def body(kernels, tile_owner, tile_source, tile_target, tile_seed, tile_count, prev_gradient, prev_step, precond):
    pos = lax.broadcasted_iota(jnp.int32, (V, T), 1)
    live = pos < tile_count
    m = lax.axis_index("mesh")
    e = lax.axis_index("ev")
    owner = tile_owner.reshape(V, T)
    x = ((owner & 3) - (m & 3)) & 3
    y = ((owner >> 2) - (m >> 2)) & 3
    z = ((tile_target >> 4) - (e >> 1)) & 3
    c = (tile_target >> 3) ^ e
    block = x * 256 + y * 64 + z * 16 + (c & 1) * 8 + (tile_target & 7)
    src = tile_source + E * lax.broadcasted_iota(jnp.int32, (V, T), 0)
    block = jnp.where(live, block, 1024)
    code = tile_seed + (src << 7) + (block << 16)
    flat = code.reshape(V * T)
    contribution = forward(flat, kernels)
    direction, table = exchange(code.reshape(1, V * T), contribution, prev_gradient, prev_step, precond)
    return direction, backward(flat, table)


def solution(mesh):
    in_specs = (
        P("ev", None, "mesh", None),
        P("ev", "mesh", None),
        P("ev", "mesh"),
        P("ev", "mesh"),
        P("ev", "mesh"),
        P("ev", "mesh"),
        P(None, "mesh", "ev", None),
        P(None, "mesh", "ev", None),
        P(None, "mesh", "ev", None),
    )
    out_specs = (P(None, "mesh", "ev", None), P("ev", None, "mesh", None))
    return jax.shard_map(body, mesh=mesh, in_specs=in_specs, out_specs=out_specs, check_vma=False)
```

```python
import jax
import jax.numpy as jnp
from jax import lax
from jax.experimental import pallas as pl
from jax.experimental.pallas import tpu as pltpu
from jax.sharding import PartitionSpec as P

C, N, E, T, V, S = 12, 128, 256, 512, 2, 84
TILES = V * T
AXES = ((0, 1, 2), (1, 2, 0), (2, 0, 1))
WEIGHT = (256, 64, 16)
HOPS = (0, 1, 2, 1)
MESH_ID = pl.DeviceIdType.MESH
FWD_UNROLL = 64
BWD_UNROLL = 64


def fill_tables(ext, table, flip):
    i = lax.broadcasted_iota(jnp.int32, (136, N), 0).astype(jnp.float32) - 4.0
    j = lax.broadcasted_iota(jnp.int32, (136, N), 1).astype(jnp.float32)
    d = i - j
    for sp in range(3):
        spread = jnp.float32(0.55) + jnp.float32(0.1) * jnp.float32(sp)
        e = jnp.exp(-d * d / (jnp.float32(2.0) * spread * spread))
        for wt in range(4):
            weight = jnp.float32(0.1) + jnp.float32(0.1) * jnp.float32(wt)
            ext[wt * 3 + sp] = weight * e
    for k in range(12):
        for o in range(7):
            off = 3 - o if flip else o - 3
            table[k * 7 + o] = ext[k, pl.ds(4 - off, N), :].astype(jnp.bfloat16)


def main_kernel(code_s, code_ref, kern_hbm, pg_hbm, ps_hbm, pc_hbm, dir_ref, out_ref,
                kern, fields, ext, table, xs, scr, con, give, take, own, s1, s2, pr, row, rows, tab,
                kern_sem, field_sem, g_s, s1_s, s2_s, p_s, r_s, ap_s, ar_s, a2_s, ad_s,
                g_r, s1_r, s2_r, p_r, r_r, ap_r, ar_r, a2_r, ad_r):
    e = lax.axis_index("ev")
    m = lax.axis_index("mesh")
    me = e * 16 + m
    at = (lax.rem(m, 4), lax.div(m, 4), lax.div(e, 2))
    core = lax.rem(e, 2)
    coord = [[a if o == 0 else lax.rem(a + o, 4) for o in range(4)] for a in at]

    def device(dx, dy, dz, other=False):
        c = 1 - core if other else core
        return {"ev": coord[2][dz] * 2 + c, "mesh": coord[1][dy] * 4 + coord[0][dx]}

    def place(k, r, i, j):
        off = [0, 0, 0]
        for axis, o in zip(AXES[k], (r, i, j)):
            off[axis] = o % 4
        return device(*off)

    partner = device(0, 0, 0, True)

    def copy(src, dst, ssem, rsem, where):
        return pltpu.make_async_remote_copy(src_ref=src, dst_ref=dst, send_sem=ssem, recv_sem=rsem,
                                            device_id=where, device_id_type=MESH_ID)

    def send(src, dst, ssem, rsem, where):
        copy(src, dst, ssem, rsem, where).start()

    def got(ref, ssem, rsem):
        copy(ref, ref, ssem, rsem, partner).wait_recv()

    def sent(ref, ssem, rsem):
        copy(ref, ref, ssem, rsem, partner).wait_send()

    load = pltpu.make_async_copy(kern_hbm, kern, kern_sem)
    load.start()
    loads = [pltpu.make_async_copy(src, fields.at[n], field_sem.at[n]) for n, src in enumerate((pg_hbm, ps_hbm, pc_hbm))]
    for one in loads:
        one.start()
    barrier = pltpu.get_barrier_semaphore()

    def greet(d, carry):
        other = lax.rem(me + d, 128)
        pl.semaphore_signal(barrier, inc=1, device_id={"ev": lax.div(other, 16), "mesh": lax.rem(other, 16)},
                            device_id_type=MESH_ID)
        return carry

    lax.fori_loop(1, 128, greet, 0)

    fill_tables(ext, table, False)
    load.wait()
    for v in range(V):
        @pl.loop(0, E // 16)
        def _(b):
            e0 = pl.multiple_of(b * 16, 16)
            for c in range(C):
                xs[pl.ds((v * E + e0) * C + c, 16, stride=C), :] = kern[v, c, pl.ds(e0, 16), :].astype(jnp.float32)

    @pl.loop(0, TILES // FWD_UNROLL)
    def _(g):
        t0 = g * FWD_UNROLL
        for u in range(FWD_UNROLL):
            w = code_s[t0 + u]
            x = xs[pl.ds(((w >> 7) & 511) * C, 16), :].astype(jnp.bfloat16)
            scr[u * 16:u * 16 + 16, :] = jnp.dot(x, table[w & 127], preferred_element_type=jnp.float32)
        for h in range(FWD_UNROLL // 16):
            r0 = pl.multiple_of(t0 + h * 16, 16)
            for c in range(C):
                con[pl.ds(r0, 16), c * N:(c + 1) * N] = scr[pl.ds(h * 256 + c, 16, stride=16), :].astype(jnp.bfloat16)

    ids = lax.broadcasted_iota(jnp.int32, (128, N), 0)
    i_of, j_of, sub = ids >> 5, (ids >> 3) & 3, ids & 7
    block = code_ref[...] >> 16
    pl.semaphore_wait(barrier, 127)

    def partial(k, r):
        a1, a2, a3 = AXES[k]
        rows_k = i_of * WEIGHT[a2] + j_of * WEIGHT[a3] + sub
        halves = []
        for core_offset in (8, 0):
            wanted = block - (r * WEIGHT[a1] + core_offset)
            halves.append(jnp.concatenate([(rows_k == wanted[:, l * N:(l + 1) * N]).astype(jnp.float32).astype(jnp.bfloat16) for l in range(8)], axis=1))
        total = jnp.dot(jnp.concatenate(halves, axis=0), con[:, k * 512:(k + 1) * 512], preferred_element_type=jnp.float32)
        for cc in range(4):
            give[k, r, :, cc * 8:cc * 8 + 8, :] = total[:128, cc * N:(cc + 1) * N].reshape(16, 8, N)
        send(give.at[k, r], take.at[k, r], g_s, g_r.at[k, r], partner)
        for cc in range(4):
            own[k, r, :, cc * 8:cc * 8 + 8, :] = total[128:, cc * N:(cc + 1) * N].reshape(16, 8, N)

    def chip_sum(k, r):
        got(take.at[k, r], g_s, g_r.at[k, r])
        own[k, r] = own[k, r] + take[k, r]
        up, down = place(k, 1, 0, 0), place(k, 3, 0, 0)
        if r == 2:
            send(own.at[k, 2, pl.ds(0, 8)], s1.at[k, 0], s1_s, s1_r.at[k, 0], up)
            send(own.at[k, 2, pl.ds(8, 8)], s1.at[k, 1], s1_s, s1_r.at[k, 1], down)
        if r == 1:
            send(own.at[k, 1, pl.ds(8, 8)], s2.at[k, 0, pl.ds(8, 8)], s2_s, s2_r.at[k, 0, 1], up)
        if r == 3:
            send(own.at[k, 3, pl.ds(0, 8)], s2.at[k, 1, pl.ds(0, 8)], s2_s, s2_r.at[k, 1, 0], down)

    steps = [(k, r) for r in (2, 1, 3, 0) for k in range(3)]
    lag = 2
    for n, (k, r) in enumerate(steps):
        partial(k, r)
        if n >= lag:
            chip_sum(*steps[n - lag])
    for k, r in steps[len(steps) - lag:]:
        chip_sum(k, r)
    for k in range(3):
        got(s1.at[k, 0], s1_s, s1_r.at[k, 0])
        own[k, 1, 0:8] = own[k, 1, 0:8] + s1[k, 0]
        send(own.at[k, 1, pl.ds(0, 8)], s2.at[k, 0, pl.ds(0, 8)], s2_s, s2_r.at[k, 0, 0], place(k, 1, 0, 0))
        got(s1.at[k, 1], s1_s, s1_r.at[k, 1])
        own[k, 3, 8:16] = own[k, 3, 8:16] + s1[k, 1]
        send(own.at[k, 3, pl.ds(8, 8)], s2.at[k, 1, pl.ds(8, 8)], s2_s, s2_r.at[k, 1, 1], place(k, 3, 0, 0))
    far_first = sorted(range(1, 16), key=lambda q: -(HOPS[q // 4] + HOPS[q % 4]))
    for k in range(3):
        for way in range(2):
            for half in range(2):
                got(s2.at[k, way, pl.ds(half * 8, 8)], s2_s, s2_r.at[k, way, half])
        own[k, 0] = own[k, 0] + s2[k, 0] + s2[k, 1]
        for q in far_first:
            send(own.at[k, 0, q], pr.at[k, q - 1], p_s, p_r.at[k], place(k, 0, q // 4, q % 4))
    parts = []
    for k in range(3):
        got(pr.at[k], p_s, p_r.at[k])
        total = own[k, 0, 0]
        for q in range(15):
            total = total + pr[k, q]
        parts.append(total)
    gradient = jnp.concatenate(parts, axis=0)
    for one in loads:
        one.wait()
    prev_g, step, cond = (fields[n].reshape(96, N) for n in range(3))
    change = gradient - prev_g
    weighted = cond * change
    lane = lax.broadcasted_iota(jnp.int32, (1, N), 1)

    def summed(v):
        v = jnp.sum(v.reshape(12, 8, N), axis=0)
        return jnp.sum(jnp.sum(v, axis=0, keepdims=True), axis=1, keepdims=True)

    mine = jnp.zeros((1, N), jnp.float32)
    for n, v in enumerate((step * change, step * gradient, weighted * gradient, weighted * change)):
        mine = jnp.where(lane == n, summed(v), mine)
    row[...] = mine
    rows[me] = mine
    everyone = [(dx, dy, dz, other) for dx in range(4) for dy in range(4) for dz in range(4) for other in (False, True)][1:]
    for dx, dy, dz, other in sorted(everyone, key=lambda o: -(HOPS[o[0]] + HOPS[o[1]] + HOPS[o[2]])):
        send(row, rows.at[me], r_s, r_r, device(dx, dy, dz, other))
    got(rows.at[pl.ds(0, 127)], r_s, r_r)
    totals = jnp.sum(rows[...], axis=0)
    curvature, slope, cross, self_ = (
        jnp.sum(jnp.where(lane == n, totals, 0.0), axis=1, keepdims=True) for n in range(4))
    alpha = slope / curvature
    beta = (cross - alpha * self_) / curvature
    scaled = cond * (gradient - alpha * change)
    direction = -(scaled + (alpha - beta) * step)
    rounded = direction.astype(jnp.bfloat16)
    for k in range(3):
        tab[k, 0, 0, 0] = rounded[k * 32:(k + 1) * 32]
    for q in far_first:
        i, j = q // 4, q % 4
        back = (-i % 4) * 4 + (-j % 4)
        for k in range(3):
            send(tab.at[k, 0, 0, 0], tab.at[k, 0, 0, back], ap_s, ap_r.at[k, back // 4], place(k, 0, i, j))
    dir_ref[...] = direction.reshape(12, 1, 8, N)
    out_ref[TILES * C:, :] = jnp.zeros((16, N), jnp.float32)

    def spread(k, rc, r, i):
        a1, a2, a3 = AXES[k]
        for j in range(4):
            base = r * WEIGHT[a1] + i * WEIGHT[a2] + j * WEIGHT[a3] + rc * 8
            piece = tab[k, rc, r, i * 4 + j].astype(jnp.float32)
            for cc in range(4):
                out_ref[pl.ds(base * C + k * 4 + cc, 8, stride=C), :] = piece[cc * 8:cc * 8 + 8]

    def across(k, r, i):
        g = pl.ds(i * 4, 4)
        send(tab.at[k, 0, r, g], tab.at[k, 1, r, g], ad_s, ad_r.at[k, r, i], partner)

    for i in (0, 1, 3, 2):
        g = pl.ds(i * 4, 4)
        for k in range(3):
            got(tab.at[k, 0, 0, pl.ds(1, 3) if i == 0 else g], ap_s, ap_r.at[k, i])
            send(tab.at[k, 0, 0, g], tab.at[k, 0, 3, g], ar_s, ar_r.at[k, i, 0], place(k, 1, 0, 0))
            send(tab.at[k, 0, 0, g], tab.at[k, 0, 1, g], ar_s, ar_r.at[k, i, 1], place(k, 3, 0, 0))
            across(k, 0, i)
            spread(k, 0, 0, i)
    for i in (0, 1, 3, 2):
        g = pl.ds(i * 4, 4)
        for k in range(3):
            for way, r in ((0, 3), (1, 1)):
                got(tab.at[k, 0, r, g], ar_s, ar_r.at[k, i, way])
                if (way == 0) == (i < 2):
                    send(tab.at[k, 0, r, g], tab.at[k, 0, 2, g], a2_s, a2_r.at[k, i], place(k, 1 if way == 0 else 3, 0, 0))
                across(k, r, i)
                spread(k, 0, r, i)
    for i in (0, 1, 3, 2):
        for k in range(3):
            got(tab.at[k, 1, 0, pl.ds(i * 4, 4)], ad_s, ad_r.at[k, 0, i])
            spread(k, 1, 0, i)
    for i in (0, 1, 3, 2):
        for k in range(3):
            got(tab.at[k, 0, 2, pl.ds(i * 4, 4)], a2_s, a2_r.at[k, i])
            across(k, 2, i)
            spread(k, 0, 2, i)
    for r in (3, 1, 2):
        for i in (0, 1, 3, 2):
            for k in range(3):
                got(tab.at[k, 1, r, pl.ds(i * 4, 4)], ad_s, ad_r.at[k, r, i])
                spread(k, 1, r, i)
    sent(give, g_s, g_r.at[0, 0])
    sent(s1, s1_s, s1_r.at[0, 0])
    sent(s2, s2_s, s2_r.at[0, 0, 0])
    sent(pr, p_s, p_r.at[0])
    sent(rows.at[pl.ds(0, 127)], r_s, r_r)
    sent(tab.at[:, 0, 0, pl.ds(1, 15)], ap_s, ap_r.at[0, 0])
    sent(tab.at[:, 0, pl.ds(0, 2)], ar_s, ar_r.at[0, 0, 0])
    sent(tab.at[:, 0, 2], a2_s, a2_r.at[0, 0])
    sent(tab.at[:, 0], ad_s, ad_r.at[0, 0, 0])


def main(flat, code, kernels, prev_gradient, prev_step, precond):
    dma = pltpu.SemaphoreType.DMA
    f32, bf16 = jnp.float32, jnp.bfloat16
    vmem = pl.BlockSpec(memory_space=pltpu.VMEM)
    return pl.pallas_call(
        main_kernel,
        out_shape=(jax.ShapeDtypeStruct((C, 1, 8, N), f32), jax.ShapeDtypeStruct((TILES * C + 16, N), f32)),
        grid_spec=pltpu.PrefetchScalarGridSpec(
            num_scalar_prefetch=1, grid=(),
            in_specs=[vmem] + [pl.BlockSpec(memory_space=pltpu.HBM)] * 4,
            out_specs=(vmem, vmem),
            scratch_shapes=[
                pltpu.VMEM((V, C, E, N), bf16), pltpu.VMEM((3, C, 1, 8, N), f32), pltpu.VMEM((12, 136, N), f32), pltpu.VMEM((S, N, N), bf16),
                pltpu.VMEM((V * E * C + 16, N), f32), pltpu.VMEM((FWD_UNROLL * 16, N), f32), pltpu.VMEM((TILES, C * N), bf16),
                pltpu.VMEM((3, 4, 16, 32, N), f32), pltpu.VMEM((3, 4, 16, 32, N), f32), pltpu.VMEM((3, 4, 16, 32, N), f32),
                pltpu.VMEM((3, 2, 8, 32, N), f32), pltpu.VMEM((3, 2, 16, 32, N), f32), pltpu.VMEM((3, 15, 32, N), f32),
                pltpu.VMEM((1, N), f32), pltpu.VMEM((128, 1, N), f32), pltpu.VMEM((3, 2, 4, 16, 32, N), bf16),
            ] + [dma, dma((3,))] + [dma] * 9 + [dma((3, 4)), dma((3, 2)), dma((3, 2, 2)), dma((3,)), dma, dma((3, 4)), dma((3, 4, 2)), dma((3, 4)), dma((3, 4, 4))]),
        compiler_params=pltpu.CompilerParams(vmem_limit_bytes=44 << 20, collective_id=0, has_side_effects=True),
        name="main",
    )(flat, code, kernels, prev_gradient, prev_step, precond)


def bwd_kernel(code, xs, out_ref, ext, table, acc0, acc1):
    fill_tables(ext, table, True)
    zero = jnp.zeros((64, N), jnp.float32)

    @pl.loop(0, (E * C) // 64)
    def _(b):
        acc0[pl.ds(pl.multiple_of(b * 64, 64), 64), :] = zero
        acc1[pl.ds(pl.multiple_of(b * 64, 64), 64), :] = zero

    @pl.loop(0, T // BWD_UNROLL)
    def _(g):
        for u in range(BWD_UNROLL):
            for v, acc in ((0, acc0), (1, acc1)):
                w = code[v * T + g * BWD_UNROLL + u]
                block = w >> 16
                live = block < TILES
                x = xs[pl.ds(jnp.where(live, block, 0) * C, 16), :].astype(jnp.bfloat16)
                y = jnp.dot(x, table[w & 127], preferred_element_type=jnp.float32)
                r = jnp.where(live, (w >> 7) & 255, E) * C
                acc[pl.ds(r, 8), :] += y[:8]
                acc[pl.ds(r + 8, 4), :] += y[8:12]

    for v, acc in ((0, acc0), (1, acc1)):
        @pl.loop(0, E // 8)
        def _(b):
            e0 = pl.multiple_of(b * 8, 8)
            for c in range(C):
                out_ref[v, c, pl.ds(e0, 8), :] = acc[pl.ds(e0 * C + c, 8, stride=C), :]


def backward(code, dirs):
    f32 = jnp.float32
    return pl.pallas_call(
        bwd_kernel,
        out_shape=jax.ShapeDtypeStruct((V, C, E, N), f32),
        grid_spec=pltpu.PrefetchScalarGridSpec(
            num_scalar_prefetch=1, grid=(),
            in_specs=[pl.BlockSpec(memory_space=pltpu.VMEM)],
            out_specs=pl.BlockSpec(memory_space=pltpu.VMEM),
            scratch_shapes=[pltpu.VMEM((12, 136, N), f32), pltpu.VMEM((S, N, N), jnp.bfloat16),
                            pltpu.VMEM((E * C + 16, N), f32), pltpu.VMEM((E * C + 16, N), f32)]),
        compiler_params=pltpu.CompilerParams(vmem_limit_bytes=44 << 20),
        name="bwd",
    )(code, dirs)


def body(kernels, tile_owner, tile_source, tile_target, tile_seed, tile_count, prev_gradient, prev_step, precond):
    live = lax.broadcasted_iota(jnp.int32, (V, T), 1) < tile_count
    m = lax.axis_index("mesh")
    e = lax.axis_index("ev")
    owner = tile_owner.reshape(V, T)
    x = ((owner & 3) - (m & 3)) & 3
    y = ((owner >> 2) - (m >> 2)) & 3
    z = ((tile_target >> 4) - (e >> 1)) & 3
    c = ((tile_target >> 3) ^ e) & 1
    block = jnp.where(live, x * 256 + y * 64 + z * 16 + c * 8 + (tile_target & 7), TILES)
    src = tile_source + E * lax.broadcasted_iota(jnp.int32, (V, T), 0)
    code = tile_seed + (src << 7) + (block << 16)
    flat = code.reshape(TILES)
    direction, dirs = main(flat, code.reshape(1, TILES), kernels, prev_gradient, prev_step, precond)
    return direction, backward(flat, dirs)


def solution(mesh):
    in_specs = (
        P("ev", None, "mesh", None),
        P("ev", "mesh", None),
        P("ev", "mesh"),
        P("ev", "mesh"),
        P("ev", "mesh"),
        P("ev", "mesh"),
        P(None, "mesh", "ev", None),
        P(None, "mesh", "ev", None),
        P(None, "mesh", "ev", None),
    )
    out_specs = (P(None, "mesh", "ev", None), P("ev", None, "mesh", None))
    return jax.shard_map(body, mesh=mesh, in_specs=in_specs, out_specs=out_specs, check_vma=False)
```

```python
import jax
import jax.numpy as jnp
from jax import lax
from jax.experimental import pallas as pl
from jax.experimental.pallas import tpu as pltpu
from jax.sharding import PartitionSpec as P

C, N, E, T, V, S = 12, 128, 256, 512, 2, 84
TILES = V * T
AXES = ((0, 1, 2), (1, 2, 0), (2, 0, 1))
WEIGHT = (256, 64, 16)
HOPS = (0, 1, 2, 1)
MESH_ID = pl.DeviceIdType.MESH
FWD_UNROLL = 128
BWD_UNROLL = 128


def fill_tables(ext, table, flip):
    i = lax.broadcasted_iota(jnp.int32, (136, N), 0).astype(jnp.float32) - 4.0
    j = lax.broadcasted_iota(jnp.int32, (136, N), 1).astype(jnp.float32)
    d = i - j
    for sp in range(3):
        spread = jnp.float32(0.55) + jnp.float32(0.1) * jnp.float32(sp)
        e = jnp.exp(-d * d / (jnp.float32(2.0) * spread * spread))
        for wt in range(4):
            weight = jnp.float32(0.1) + jnp.float32(0.1) * jnp.float32(wt)
            ext[wt * 3 + sp] = weight * e
    for k in range(12):
        for o in range(7):
            off = 3 - o if flip else o - 3
            table[k * 7 + o] = ext[k, pl.ds(4 - off, N), :].astype(jnp.bfloat16)


def main_kernel(code_s, code_ref, kern_hbm, pg_hbm, ps_hbm, pc_hbm, dir_ref, out_ref,
                kern, fields, ext, table, xs, scr, con, give, take, own, s1, s2, pr, row, rows, tab,
                kern_sem, field_sem, g_s, s1_s, s2_s, p_s, r_s, ap_s, ar_s, a2_s, ad_s,
                g_r, s1_r, s2_r, d2_r, p_r, r_r, ap_r, ar_r, a2_r, ad_r):
    e = lax.axis_index("ev")
    m = lax.axis_index("mesh")
    me = e * 16 + m
    at = (lax.rem(m, 4), lax.div(m, 4), lax.div(e, 2))
    core = lax.rem(e, 2)
    coord = [[a if o == 0 else lax.rem(a + o, 4) for o in range(4)] for a in at]

    ev_of = [(z * 2 + core, z * 2 + (1 - core)) for z in coord[2]]
    mesh_of = [[y * 4 + x for x in coord[0]] for y in coord[1]]

    def device(dx, dy, dz, other=False):
        return {"ev": ev_of[dz][int(other)], "mesh": mesh_of[dy][dx]}

    def place(k, r, i, j):
        off = [0, 0, 0]
        for axis, o in zip(AXES[k], (r, i, j)):
            off[axis] = o % 4
        return device(*off)

    partner = device(0, 0, 0, True)

    def copy(src, dst, ssem, rsem, where):
        return pltpu.make_async_remote_copy(src_ref=src, dst_ref=dst, send_sem=ssem, recv_sem=rsem,
                                            device_id=where, device_id_type=MESH_ID)

    def send(src, dst, ssem, rsem, where):
        copy(src, dst, ssem, rsem, where).start()

    def got(ref, ssem, rsem):
        copy(ref, ref, ssem, rsem, partner).wait_recv()

    def sent(ref, ssem, rsem):
        copy(ref, ref, ssem, rsem, partner).wait_send()

    load = pltpu.make_async_copy(kern_hbm, kern, kern_sem)
    load.start()
    loads = [pltpu.make_async_copy(src, fields.at[n], field_sem.at[n]) for n, src in enumerate((pg_hbm, ps_hbm, pc_hbm))]
    for one in loads:
        one.start()
    barrier = pltpu.get_barrier_semaphore()

    everyone = [(dx, dy, dz, other) for dx in range(4) for dy in range(4) for dz in range(4) for other in (False, True)][1:]
    everyone.sort(key=lambda o: -(HOPS[o[0]] + HOPS[o[1]] + HOPS[o[2]]))
    for dx, dy, dz, other in everyone:
        pl.semaphore_signal(barrier, inc=1, device_id=device(dx, dy, dz, other), device_id_type=MESH_ID)

    fill_tables(ext, table, False)
    load.wait()
    for v in range(V):
        @pl.loop(0, E // 16)
        def _(b):
            e0 = pl.multiple_of(b * 16, 16)
            for c in range(C):
                xs[pl.ds((v * E + e0) * C + c, 16, stride=C), :] = kern[v, c, pl.ds(e0, 16), :].astype(jnp.float32)

    @pl.loop(0, TILES // FWD_UNROLL)
    def _(g):
        t0 = g * FWD_UNROLL
        for u in range(FWD_UNROLL):
            w = code_s[t0 + u]
            x = xs[pl.ds(((w >> 7) & 511) * C, 16), :].astype(jnp.bfloat16)
            scr[u * 16:u * 16 + 16, :] = jnp.dot(x, table[w & 127], preferred_element_type=jnp.float32)
        for h in range(FWD_UNROLL // 16):
            r0 = pl.multiple_of(t0 + h * 16, 16)
            for c in range(C):
                con[pl.ds(r0, 16), c * N:(c + 1) * N] = scr[pl.ds(h * 256 + c, 16, stride=16), :].astype(jnp.bfloat16)

    ids = lax.broadcasted_iota(jnp.int32, (128, N), 0)
    i_of, j_of, sub = ids >> 5, (ids >> 3) & 3, ids & 7
    block = code_ref[...] >> 16
    pl.semaphore_wait(barrier, 127)

    def partial(k, r):
        a1, a2, a3 = AXES[k]
        rows_k = i_of * WEIGHT[a2] + j_of * WEIGHT[a3] + sub
        halves = []
        for core_offset in (8, 0):
            wanted = block - (r * WEIGHT[a1] + core_offset)
            halves.append(jnp.concatenate([(rows_k == wanted[:, l * N:(l + 1) * N]).astype(jnp.float32).astype(jnp.bfloat16) for l in range(8)], axis=1))
        total = jnp.dot(jnp.concatenate(halves, axis=0), con[:, k * 512:(k + 1) * 512], preferred_element_type=jnp.float32)
        for cc in range(4):
            give[k, r, :, cc * 8:cc * 8 + 8, :] = total[:128, cc * N:(cc + 1) * N].reshape(16, 8, N)
        send(give.at[k, r], take.at[k, r], g_s, g_r.at[k, r], partner)
        for cc in range(4):
            own[k, r, :, cc * 8:cc * 8 + 8, :] = total[128:, cc * N:(cc + 1) * N].reshape(16, 8, N)

    def chip_sum(k, r):
        got(take.at[k, r], g_s, g_r.at[k, r])
        own[k, r] = own[k, r] + take[k, r]
        up, down = place(k, 1, 0, 0), place(k, 3, 0, 0)
        if r == 2:
            for i in (1, 2, 0, 3):
                send(own.at[k, 2, pl.ds(i * 4, 4)], s1.at[k, i], s1_s, s1_r.at[k, i], up if i < 2 else down)
        if r == 1:
            send(own.at[k, 1, pl.ds(8, 8)], s2.at[k, 0, pl.ds(8, 8)], s2_s, d2_r.at[k, 0], up)
        if r == 3:
            send(own.at[k, 3, pl.ds(0, 8)], s2.at[k, 1, pl.ds(0, 8)], s2_s, d2_r.at[k, 1], down)

    steps = [(k, r) for r in (2, 1, 3, 0) for k in range(3)]
    lag = 2
    for n, (k, r) in enumerate(steps):
        partial(k, r)
        if n >= lag:
            chip_sum(*steps[n - lag])
    for k, r in steps[len(steps) - lag:]:
        chip_sum(k, r)
    for i in (1, 2, 0, 3):
        g = pl.ds(i * 4, 4)
        for k in range(3):
            r, way = (1, 0) if i < 2 else (3, 1)
            got(s1.at[k, i], s1_s, s1_r.at[k, i])
            own[k, r, g] = own[k, r, g] + s1[k, i]
            send(own.at[k, r, g], s2.at[k, way, g], s2_s, s2_r.at[k, i], place(k, r, 0, 0))
    far_first = sorted(range(1, 16), key=lambda q: -(HOPS[q // 4] + HOPS[q % 4]))
    for i in (1, 2, 0, 3):
        g = pl.ds(i * 4, 4)
        for k in range(3):
            if i == 1:
                got(s2.at[k, 0, pl.ds(8, 8)], s2_s, d2_r.at[k, 0])
                got(s2.at[k, 1, pl.ds(0, 8)], s2_s, d2_r.at[k, 1])
            got(s2.at[k, 0 if i < 2 else 1, g], s2_s, s2_r.at[k, i])
            own[k, 0, g] = own[k, 0, g] + s2[k, 0, g] + s2[k, 1, g]
            for q in far_first:
                if q // 4 == i:
                    send(own.at[k, 0, q], pr.at[k, q - 1], p_s, p_r.at[k], place(k, 0, i, q % 4))
    parts = []
    for k in range(3):
        got(pr.at[k], p_s, p_r.at[k])
        total = own[k, 0, 0]
        for q in range(15):
            total = total + pr[k, q]
        parts.append(total)
    gradient = jnp.concatenate(parts, axis=0)
    for one in loads:
        one.wait()
    prev_g, step, cond = (fields[n].reshape(96, N) for n in range(3))
    change = gradient - prev_g
    weighted = cond * change
    lane = lax.broadcasted_iota(jnp.int32, (1, N), 1)

    def summed(v):
        v = jnp.sum(v.reshape(12, 8, N), axis=0)
        return jnp.sum(jnp.sum(v, axis=0, keepdims=True), axis=1, keepdims=True)

    mine = jnp.zeros((1, N), jnp.float32)
    for n, v in enumerate((step * change, step * gradient, weighted * gradient, weighted * change)):
        mine = jnp.where(lane == n, summed(v), mine)
    row[...] = mine
    rows[me] = mine
    for dx, dy, dz, other in everyone:
        send(row, rows.at[me], r_s, r_r, device(dx, dy, dz, other))
    got(rows.at[pl.ds(0, 127)], r_s, r_r)
    totals = jnp.sum(rows[...], axis=0)
    curvature, slope, cross, self_ = (
        jnp.sum(jnp.where(lane == n, totals, 0.0), axis=1, keepdims=True) for n in range(4))
    alpha = slope / curvature
    beta = (cross - alpha * self_) / curvature
    scaled = cond * (gradient - alpha * change)
    direction = -(scaled + (alpha - beta) * step)
    rounded = direction.astype(jnp.bfloat16)
    for k in range(3):
        tab[k, 0, 0, 0] = rounded[k * 32:(k + 1) * 32]
    for q in far_first:
        i, j = q // 4, q % 4
        back = (-i % 4) * 4 + (-j % 4)
        for k in range(3):
            send(tab.at[k, 0, 0, 0], tab.at[k, 0, 0, back], ap_s, ap_r.at[k, back // 4], place(k, 0, i, j))
    dir_ref[...] = direction.reshape(12, 1, 8, N)
    out_ref[TILES * C:, :] = jnp.zeros((16, N), jnp.float32)

    def spread(k, rc, r, i):
        a1, a2, a3 = AXES[k]
        for j in range(4):
            base = r * WEIGHT[a1] + i * WEIGHT[a2] + j * WEIGHT[a3] + rc * 8
            piece = tab[k, rc, r, i * 4 + j].astype(jnp.float32)
            for cc in range(4):
                out_ref[pl.ds(base * C + k * 4 + cc, 8, stride=C), :] = piece[cc * 8:cc * 8 + 8]

    def across(k, r, i):
        g = pl.ds(i * 4, 4)
        send(tab.at[k, 0, r, g], tab.at[k, 1, r, g], ad_s, ad_r.at[k, r, i], partner)

    for i in (0, 1, 3, 2):
        g = pl.ds(i * 4, 4)
        for k in range(3):
            got(tab.at[k, 0, 0, pl.ds(1, 3) if i == 0 else g], ap_s, ap_r.at[k, i])
            send(tab.at[k, 0, 0, g], tab.at[k, 0, 3, g], ar_s, ar_r.at[k, i, 0], place(k, 1, 0, 0))
            send(tab.at[k, 0, 0, g], tab.at[k, 0, 1, g], ar_s, ar_r.at[k, i, 1], place(k, 3, 0, 0))
            if i == 2:
                send(tab.at[k, 0, 0, g], tab.at[k, 0, 2, g], a2_s, a2_r.at[k, i], place(k, 2, 0, 0))
            across(k, 0, i)
            spread(k, 0, 0, i)
    for i in (0, 1, 3, 2):
        g = pl.ds(i * 4, 4)
        for k in range(3):
            for way, r in ((0, 3), (1, 1)):
                got(tab.at[k, 0, r, g], ar_s, ar_r.at[k, i, way])
                if i != 2 and (way == 0) == (i < 2):
                    send(tab.at[k, 0, r, g], tab.at[k, 0, 2, g], a2_s, a2_r.at[k, i], place(k, 1 if way == 0 else 3, 0, 0))
                across(k, r, i)
                spread(k, 0, r, i)
    for i in (0, 1, 3, 2):
        for k in range(3):
            got(tab.at[k, 1, 0, pl.ds(i * 4, 4)], ad_s, ad_r.at[k, 0, i])
            spread(k, 1, 0, i)
    for i in (0, 1, 3, 2):
        for k in range(3):
            got(tab.at[k, 0, 2, pl.ds(i * 4, 4)], a2_s, a2_r.at[k, i])
            across(k, 2, i)
            spread(k, 0, 2, i)
    for r in (3, 1, 2):
        for i in (0, 1, 3, 2):
            for k in range(3):
                got(tab.at[k, 1, r, pl.ds(i * 4, 4)], ad_s, ad_r.at[k, r, i])
                spread(k, 1, r, i)
    sent(give, g_s, g_r.at[0, 0])
    sent(s1, s1_s, s1_r.at[0, 0])
    sent(s2, s2_s, s2_r.at[0, 0])
    sent(pr, p_s, p_r.at[0])
    sent(rows.at[pl.ds(0, 127)], r_s, r_r)
    sent(tab.at[:, 0, 0, pl.ds(1, 15)], ap_s, ap_r.at[0, 0])
    sent(tab.at[:, 0, pl.ds(0, 2)], ar_s, ar_r.at[0, 0, 0])
    sent(tab.at[:, 0, 2], a2_s, a2_r.at[0, 0])
    sent(tab.at[:, 0], ad_s, ad_r.at[0, 0, 0])


def main(flat, code, kernels, prev_gradient, prev_step, precond):
    dma = pltpu.SemaphoreType.DMA
    f32, bf16 = jnp.float32, jnp.bfloat16
    vmem = pl.BlockSpec(memory_space=pltpu.VMEM)
    return pl.pallas_call(
        main_kernel,
        out_shape=(jax.ShapeDtypeStruct((C, 1, 8, N), f32), jax.ShapeDtypeStruct((TILES * C + 16, N), f32)),
        grid_spec=pltpu.PrefetchScalarGridSpec(
            num_scalar_prefetch=1, grid=(),
            in_specs=[vmem] + [pl.BlockSpec(memory_space=pltpu.HBM)] * 4,
            out_specs=(vmem, vmem),
            scratch_shapes=[
                pltpu.VMEM((V, C, E, N), bf16), pltpu.VMEM((3, C, 1, 8, N), f32), pltpu.VMEM((12, 136, N), f32), pltpu.VMEM((S, N, N), bf16),
                pltpu.VMEM((V * E * C + 16, N), f32), pltpu.VMEM((FWD_UNROLL * 16, N), f32), pltpu.VMEM((TILES, C * N), bf16),
                pltpu.VMEM((3, 4, 16, 32, N), f32), pltpu.VMEM((3, 4, 16, 32, N), f32), pltpu.VMEM((3, 4, 16, 32, N), f32),
                pltpu.VMEM((3, 4, 4, 32, N), f32), pltpu.VMEM((3, 2, 16, 32, N), f32), pltpu.VMEM((3, 15, 32, N), f32),
                pltpu.VMEM((1, N), f32), pltpu.VMEM((128, 1, N), f32), pltpu.VMEM((3, 2, 4, 16, 32, N), bf16),
            ] + [dma, dma((3,))] + [dma] * 9 + [dma((3, 4)), dma((3, 4)), dma((3, 4)), dma((3, 2)), dma((3,)), dma, dma((3, 4)), dma((3, 4, 2)), dma((3, 4)), dma((3, 4, 4))]),
        compiler_params=pltpu.CompilerParams(vmem_limit_bytes=44 << 20, collective_id=0, has_side_effects=True),
        name="main",
    )(flat, code, *(pltpu.with_memory_space_constraint(v, pltpu.HBM) for v in (kernels, prev_gradient, prev_step, precond)))


def bwd_kernel(code, xs, dir_ref, out_ref, dir_out, ext, table, acc0, acc1, stage, sem):
    fill_tables(ext, table, True)
    zero = jnp.zeros((64, N), jnp.float32)

    @pl.loop(0, (E * C) // 64)
    def _(b):
        acc0[pl.ds(pl.multiple_of(b * 64, 64), 64), :] = zero
        acc1[pl.ds(pl.multiple_of(b * 64, 64), 64), :] = zero

    @pl.loop(0, T // BWD_UNROLL)
    def _(g):
        for u in range(BWD_UNROLL):
            for v, acc in ((0, acc0), (1, acc1)):
                w = code[v * T + g * BWD_UNROLL + u]
                block = w >> 16
                live = block < TILES
                x = xs[pl.ds(jnp.where(live, block, 0) * C, 16), :].astype(jnp.bfloat16)
                y = jnp.dot(x, table[w & 127], preferred_element_type=jnp.float32)
                r = jnp.where(live, (w >> 7) & 255, E) * C
                acc[pl.ds(r, 8), :] += y[:8]
                acc[pl.ds(r + 8, 4), :] += y[8:12]

    def leave(n):
        return pltpu.make_async_copy(stage.at[n], out_ref.at[n // 4, :, pl.ds(n % 4 * 64, 64)], sem.at[n])

    for n in range(8):
        acc = (acc0, acc1)[n // 4]

        @pl.loop(0, 8)
        def _(b):
            e0 = pl.multiple_of(b * 8, 8)
            for c in range(C):
                stage[n, c, pl.ds(e0, 8), :] = acc[pl.ds((n % 4 * 64 + e0) * C + c, 8, stride=C), :]

        leave(n).start()
    dir_out[...] = dir_ref[...]
    for n in range(8):
        leave(n).wait()


def backward(code, dirs, direction):
    f32 = jnp.float32
    return pl.pallas_call(
        bwd_kernel,
        out_shape=(jax.ShapeDtypeStruct((V, C, E, N), f32), jax.ShapeDtypeStruct((C, 1, 8, N), f32)),
        grid_spec=pltpu.PrefetchScalarGridSpec(
            num_scalar_prefetch=1, grid=(),
            in_specs=[pl.BlockSpec(memory_space=pltpu.VMEM)] * 2,
            out_specs=(pl.BlockSpec(memory_space=pl.ANY), pl.BlockSpec(memory_space=pltpu.VMEM)),
            scratch_shapes=[pltpu.VMEM((12, 136, N), f32), pltpu.VMEM((S, N, N), jnp.bfloat16),
                            pltpu.VMEM((E * C + 16, N), f32), pltpu.VMEM((E * C + 16, N), f32),
                            pltpu.VMEM((8, C, 64, N), f32), pltpu.SemaphoreType.DMA((8,))]),
        compiler_params=pltpu.CompilerParams(vmem_limit_bytes=44 << 20),
        name="bwd",
    )(code, dirs, direction)


def body(kernels, tile_owner, tile_source, tile_target, tile_seed, tile_count, prev_gradient, prev_step, precond):
    live = lax.broadcasted_iota(jnp.int32, (V, T), 1) < tile_count
    m = lax.axis_index("mesh")
    e = lax.axis_index("ev")
    owner = tile_owner.reshape(V, T)
    x = ((owner & 3) - (m & 3)) & 3
    y = ((owner >> 2) - (m >> 2)) & 3
    z = ((tile_target >> 4) - (e >> 1)) & 3
    c = ((tile_target >> 3) ^ e) & 1
    block = jnp.where(live, x * 256 + y * 64 + z * 16 + c * 8 + (tile_target & 7), TILES)
    src = tile_source + E * lax.broadcasted_iota(jnp.int32, (V, T), 0)
    code = tile_seed + (src << 7) + (block << 16)
    flat = code.reshape(TILES)
    direction, dirs = main(flat, code.reshape(1, TILES), kernels, prev_gradient, prev_step, precond)
    event_direction, direction = backward(flat, dirs, direction)
    return direction, event_direction


def solution(mesh):
    in_specs = (
        P("ev", None, "mesh", None),
        P("ev", "mesh", None),
        P("ev", "mesh"),
        P("ev", "mesh"),
        P("ev", "mesh"),
        P("ev", "mesh"),
        P(None, "mesh", "ev", None),
        P(None, "mesh", "ev", None),
        P(None, "mesh", "ev", None),
    )
    out_specs = (P(None, "mesh", "ev", None), P("ev", None, "mesh", None))
    return jax.shard_map(body, mesh=mesh, in_specs=in_specs, out_specs=out_specs, check_vma=False)
```

```python
import jax
import jax.numpy as jnp
from jax import lax
from jax.experimental import pallas as pl
from jax.experimental.pallas import tpu as pltpu
from jax.sharding import PartitionSpec as P

C, N, E, T, V, S = 12, 128, 256, 512, 2, 84
TILES = V * T
AXES = ((0, 1, 2), (1, 2, 0), (2, 0, 1))
WEIGHT = (256, 64, 16)
HOPS = (0, 1, 2, 1)
MESH_ID = pl.DeviceIdType.MESH
FWD_UNROLL = 256
BWD_UNROLL = 128


def fill_tables(ext, table, flip):
    i = lax.broadcasted_iota(jnp.int32, (136, N), 0).astype(jnp.float32) - 4.0
    j = lax.broadcasted_iota(jnp.int32, (136, N), 1).astype(jnp.float32)
    d = i - j
    for sp in range(3):
        spread = jnp.float32(0.55) + jnp.float32(0.1) * jnp.float32(sp)
        e = jnp.exp(-d * d / (jnp.float32(2.0) * spread * spread))
        for wt in range(4):
            weight = jnp.float32(0.1) + jnp.float32(0.1) * jnp.float32(wt)
            ext[wt * 3 + sp] = weight * e
    for k in range(12):
        for o in range(7):
            off = 3 - o if flip else o - 3
            table[k * 7 + o] = ext[k, pl.ds(4 - off, N), :].astype(jnp.bfloat16)


def main_kernel(count_hbm, kern_hbm, owner_hbm, target_hbm, seed_hbm, source_hbm, pg_hbm, ps_hbm, pc_hbm, dir_ref, out_ref, code_ref,
                seed_s, source_s, count, owner, words, kern, fields, ext, table, xs, scr, con, give, take, own, s1, s2, pr, row, rows, tab,
                kern_sem, word_sem, field_sem, g_s, s1_s, s2_s, p_s, r_s, ap_s, ar_s, a2_s, ad_s,
                g_r, s1_r, s2_r, d2_r, p_r, r_r, ap_r, ar_r, a2_r, ad_r):
    e = lax.axis_index("ev")
    m = lax.axis_index("mesh")
    me = e * 16 + m
    at = (lax.rem(m, 4), lax.div(m, 4), lax.div(e, 2))
    core = lax.rem(e, 2)
    coord = [[a if o == 0 else lax.rem(a + o, 4) for o in range(4)] for a in at]

    ev_of = [(z * 2 + core, z * 2 + (1 - core)) for z in coord[2]]
    mesh_of = [[y * 4 + x for x in coord[0]] for y in coord[1]]

    def device(dx, dy, dz, other=False):
        return {"ev": ev_of[dz][int(other)], "mesh": mesh_of[dy][dx]}

    def place(k, r, i, j):
        off = [0, 0, 0]
        for axis, o in zip(AXES[k], (r, i, j)):
            off[axis] = o % 4
        return device(*off)

    partner = device(0, 0, 0, True)

    def copy(src, dst, ssem, rsem, where):
        return pltpu.make_async_remote_copy(src_ref=src, dst_ref=dst, send_sem=ssem, recv_sem=rsem,
                                            device_id=where, device_id_type=MESH_ID)

    def send(src, dst, ssem, rsem, where):
        copy(src, dst, ssem, rsem, where).start()

    def got(ref, ssem, rsem):
        copy(ref, ref, ssem, rsem, partner).wait_recv()

    def sent(ref, ssem, rsem):
        copy(ref, ref, ssem, rsem, partner).wait_send()

    load = pltpu.make_async_copy(kern_hbm, kern, kern_sem)
    load.start()
    indices = [pltpu.make_async_copy(src, dst, word_sem.at[n]) for n, (src, dst) in enumerate((
        (seed_hbm, seed_s), (source_hbm, source_s), (owner_hbm, owner), (target_hbm, words.at[0]), (seed_hbm, words.at[1]), (source_hbm, words.at[2]), (count_hbm, count)))]
    for one in indices:
        one.start()
    loads = [pltpu.make_async_copy(src, fields.at[n], field_sem.at[n]) for n, src in enumerate((pg_hbm, ps_hbm, pc_hbm))]
    for one in loads:
        one.start()
    barrier = pltpu.get_barrier_semaphore()

    everyone = [(dx, dy, dz, other) for dx in range(4) for dy in range(4) for dz in range(4) for other in (False, True)][1:]
    everyone.sort(key=lambda o: -(HOPS[o[0]] + HOPS[o[1]] + HOPS[o[2]]))
    for dx, dy, dz, other in everyone:
        pl.semaphore_signal(barrier, inc=1, device_id=device(dx, dy, dz, other), device_id_type=MESH_ID)

    fill_tables(ext, table, False)
    load.wait()
    for one in indices:
        one.wait()
    lanes = lax.broadcasted_iota(jnp.int32, (1, T), 1)
    blocks = []
    for v in range(V):
        home, goal = owner[v], words[0, v:v + 1, :]
        dx = ((home & 3) - at[0]) & 3
        dy = ((home >> 2) - at[1]) & 3
        dz = ((goal >> 4) - at[2]) & 3
        dc = ((goal >> 3) - core) & 1
        block = dx * 256 + dy * 64 + dz * 16 + dc * 8 + (goal & 7)
        block = jnp.where(lanes < count[0:1, v:v + 1], block, TILES)
        code_ref[v:v + 1, :] = words[1, v:v + 1, :] + (words[2, v:v + 1, :] << 7) + (block << 16)
        blocks.append(block)
    for v in range(V):
        @pl.loop(0, E // 16)
        def _(b):
            e0 = pl.multiple_of(b * 16, 16)
            for c in range(C):
                xs[pl.ds((v * E + e0) * C + c, 16, stride=C), :] = kern[v, c, pl.ds(e0, 16), :].astype(jnp.float32)

    @pl.loop(0, TILES // FWD_UNROLL)
    def _(g):
        t0 = g * FWD_UNROLL
        for u in range(FWD_UNROLL):
            t = (g % (T // FWD_UNROLL)) * FWD_UNROLL + u
            v = g // (T // FWD_UNROLL)
            x = xs[pl.ds((v * E + source_s[v, t]) * C, 16), :].astype(jnp.bfloat16)
            scr[u * 16:u * 16 + 16, :] = jnp.dot(x, table[seed_s[v, t]], preferred_element_type=jnp.float32)
        for h in range(FWD_UNROLL // 16):
            r0 = pl.multiple_of(t0 + h * 16, 16)
            for c in range(C):
                con[pl.ds(r0, 16), c * N:(c + 1) * N] = scr[pl.ds(h * 256 + c, 16, stride=16), :].astype(jnp.bfloat16)

    ids = lax.broadcasted_iota(jnp.int32, (128, N), 0)
    i_of, j_of, sub = ids >> 5, (ids >> 3) & 3, ids & 7
    block = jnp.concatenate(blocks, axis=1)
    pl.semaphore_wait(barrier, 127)

    def partial(k, r):
        a1, a2, a3 = AXES[k]
        rows_k = i_of * WEIGHT[a2] + j_of * WEIGHT[a3] + sub
        halves = []
        for core_offset in (8, 0):
            wanted = block - (r * WEIGHT[a1] + core_offset)
            halves.append(jnp.concatenate([(rows_k == wanted[:, l * N:(l + 1) * N]).astype(jnp.float32).astype(jnp.bfloat16) for l in range(8)], axis=1))
        total = jnp.dot(jnp.concatenate(halves, axis=0), con[:, k * 512:(k + 1) * 512], preferred_element_type=jnp.float32)
        for cc in range(4):
            give[k, r, :, cc * 8:cc * 8 + 8, :] = total[:128, cc * N:(cc + 1) * N].reshape(16, 8, N)
        send(give.at[k, r], take.at[k, r], g_s, g_r.at[k, r], partner)
        for cc in range(4):
            own[k, r, :, cc * 8:cc * 8 + 8, :] = total[128:, cc * N:(cc + 1) * N].reshape(16, 8, N)

    def chip_sum(k, r):
        got(take.at[k, r], g_s, g_r.at[k, r])
        own[k, r] = own[k, r] + take[k, r]
        up, down = place(k, 1, 0, 0), place(k, 3, 0, 0)
        if r == 2:
            for i in (1, 2, 0, 3):
                send(own.at[k, 2, pl.ds(i * 4, 4)], s1.at[k, i], s1_s, s1_r.at[k, i], up if i < 2 else down)
        if r == 1:
            send(own.at[k, 1, pl.ds(8, 8)], s2.at[k, 0, pl.ds(8, 8)], s2_s, d2_r.at[k, 0], up)
        if r == 3:
            send(own.at[k, 3, pl.ds(0, 8)], s2.at[k, 1, pl.ds(0, 8)], s2_s, d2_r.at[k, 1], down)

    steps = [(k, r) for r in (2, 1, 3, 0) for k in range(3)]
    lag = 2
    for n, (k, r) in enumerate(steps):
        partial(k, r)
        if n >= lag:
            chip_sum(*steps[n - lag])
    for k, r in steps[len(steps) - lag:]:
        chip_sum(k, r)
    for i in (1, 2, 0, 3):
        g = pl.ds(i * 4, 4)
        for k in range(3):
            r, way = (1, 0) if i < 2 else (3, 1)
            got(s1.at[k, i], s1_s, s1_r.at[k, i])
            own[k, r, g] = own[k, r, g] + s1[k, i]
            send(own.at[k, r, g], s2.at[k, way, g], s2_s, s2_r.at[k, i], place(k, r, 0, 0))
    far_first = sorted(range(1, 16), key=lambda q: -(HOPS[q // 4] + HOPS[q % 4]))
    for i in (1, 2, 0, 3):
        g = pl.ds(i * 4, 4)
        for k in range(3):
            if i == 1:
                got(s2.at[k, 0, pl.ds(8, 8)], s2_s, d2_r.at[k, 0])
                got(s2.at[k, 1, pl.ds(0, 8)], s2_s, d2_r.at[k, 1])
            got(s2.at[k, 0 if i < 2 else 1, g], s2_s, s2_r.at[k, i])
            own[k, 0, g] = own[k, 0, g] + s2[k, 0, g] + s2[k, 1, g]
            for q in far_first:
                if q // 4 == i:
                    send(own.at[k, 0, q], pr.at[k, q - 1], p_s, p_r.at[k], place(k, 0, i, q % 4))
    parts = []
    for k in range(3):
        got(pr.at[k], p_s, p_r.at[k])
        total = own[k, 0, 0]
        for q in range(15):
            total = total + pr[k, q]
        parts.append(total)
    gradient = jnp.concatenate(parts, axis=0)
    for one in loads:
        one.wait()
    prev_g, step, cond = (fields[n].reshape(96, N) for n in range(3))
    change = gradient - prev_g
    weighted = cond * change
    lane = lax.broadcasted_iota(jnp.int32, (1, N), 1)

    def summed(v):
        v = jnp.sum(v.reshape(12, 8, N), axis=0)
        return jnp.sum(jnp.sum(v, axis=0, keepdims=True), axis=1, keepdims=True)

    mine = jnp.zeros((1, N), jnp.float32)
    for n, v in enumerate((step * change, step * gradient, weighted * gradient, weighted * change)):
        mine = jnp.where(lane == n, summed(v), mine)
    row[...] = mine
    rows[me] = mine
    for dx, dy, dz, other in everyone:
        send(row, rows.at[me], r_s, r_r, device(dx, dy, dz, other))
    got(rows.at[pl.ds(0, 127)], r_s, r_r)
    totals = jnp.sum(rows[...], axis=0)
    curvature, slope, cross, self_ = (
        jnp.sum(jnp.where(lane == n, totals, 0.0), axis=1, keepdims=True) for n in range(4))
    alpha = slope / curvature
    beta = (cross - alpha * self_) / curvature
    scaled = cond * (gradient - alpha * change)
    direction = -(scaled + (alpha - beta) * step)
    rounded = direction.astype(jnp.bfloat16)
    for k in range(3):
        tab[k, 0, 0, 0] = rounded[k * 32:(k + 1) * 32]
    for q in far_first:
        i, j = q // 4, q % 4
        back = (-i % 4) * 4 + (-j % 4)
        for k in range(3):
            send(tab.at[k, 0, 0, 0], tab.at[k, 0, 0, back], ap_s, ap_r.at[k, back // 4], place(k, 0, i, j))

    dir_ref[...] = direction.reshape(12, 1, 8, N)
    out_ref[TILES * C:, :] = jnp.zeros((16, N), jnp.float32)

    def spread(k, rc, r, i):
        a1, a2, a3 = AXES[k]
        for j in range(4):
            base = r * WEIGHT[a1] + i * WEIGHT[a2] + j * WEIGHT[a3] + rc * 8
            piece = tab[k, rc, r, i * 4 + j].astype(jnp.float32)
            for cc in range(4):
                out_ref[pl.ds(base * C + k * 4 + cc, 8, stride=C), :] = piece[cc * 8:cc * 8 + 8]

    def across(k, r, i):
        g = pl.ds(i * 4, 4)
        send(tab.at[k, 0, r, g], tab.at[k, 1, r, g], ad_s, ad_r.at[k, r, i], partner)

    for i in (0, 1, 3, 2):
        g = pl.ds(i * 4, 4)
        for k in range(3):
            got(tab.at[k, 0, 0, pl.ds(1, 3) if i == 0 else g], ap_s, ap_r.at[k, i])
            send(tab.at[k, 0, 0, g], tab.at[k, 0, 2, g], a2_s, a2_r.at[k, i], place(k, 2, 0, 0))
            send(tab.at[k, 0, 0, g], tab.at[k, 0, 3, g], ar_s, ar_r.at[k, i, 0], place(k, 1, 0, 0))
            send(tab.at[k, 0, 0, g], tab.at[k, 0, 1, g], ar_s, ar_r.at[k, i, 1], place(k, 3, 0, 0))
            across(k, 0, i)
            spread(k, 0, 0, i)
    for i in (0, 1, 3, 2):
        g = pl.ds(i * 4, 4)
        for way, r in ((0, 3), (1, 1), (2, 2)):
            for k in range(3):
                got(tab.at[k, 0, r, g], ar_s, a2_r.at[k, i] if way == 2 else ar_r.at[k, i, way])
                across(k, r, i)
    for r in (0, 3, 1, 2):
        for i in (0, 1, 3, 2):
            for k in range(3):
                if r:
                    spread(k, 0, r, i)
    for r in (0, 3, 1, 2):
        for i in (0, 1, 3, 2):
            for k in range(3):
                got(tab.at[k, 1, r, pl.ds(i * 4, 4)], ad_s, ad_r.at[k, r, i])
                spread(k, 1, r, i)
    sent(give, g_s, g_r.at[0, 0])
    sent(s1, s1_s, s1_r.at[0, 0])
    sent(s2, s2_s, s2_r.at[0, 0])
    sent(pr, p_s, p_r.at[0])
    sent(rows.at[pl.ds(0, 127)], r_s, r_r)
    sent(tab.at[:, 0, 0, pl.ds(1, 15)], ap_s, ap_r.at[0, 0])
    sent(tab.at[:, 0, pl.ds(0, 2)], ar_s, ar_r.at[0, 0, 0])
    sent(tab.at[:, 0, 2], a2_s, a2_r.at[0, 0])
    sent(tab.at[:, 0], ad_s, ad_r.at[0, 0, 0])


def main(*arrays):
    dma = pltpu.SemaphoreType.DMA
    f32, bf16, i32 = jnp.float32, jnp.bfloat16, jnp.int32
    vmem = pl.BlockSpec(memory_space=pltpu.VMEM)
    return pl.pallas_call(
        main_kernel,
        out_shape=(jax.ShapeDtypeStruct((C, 1, 8, N), f32), jax.ShapeDtypeStruct((TILES * C + 16, N), f32), jax.ShapeDtypeStruct((V, T), i32)),
        grid_spec=pltpu.PrefetchScalarGridSpec(
            num_scalar_prefetch=0, grid=(),
            in_specs=[pl.BlockSpec(memory_space=pltpu.HBM)] * len(arrays),
            out_specs=(vmem, vmem, vmem),
            scratch_shapes=[
                pltpu.SMEM((V, T), i32), pltpu.SMEM((V, T), i32), pltpu.VMEM((1, V), i32), pltpu.VMEM((V, 1, T), i32), pltpu.VMEM((3, V, T), i32),
                pltpu.VMEM((V, C, E, N), bf16), pltpu.VMEM((3, C, 1, 8, N), f32), pltpu.VMEM((12, 136, N), f32), pltpu.VMEM((S, N, N), bf16),
                pltpu.VMEM((V * E * C + 16, N), f32), pltpu.VMEM((FWD_UNROLL * 16, N), f32), pltpu.VMEM((TILES, C * N), bf16),
                pltpu.VMEM((3, 4, 16, 32, N), f32), pltpu.VMEM((3, 4, 16, 32, N), f32), pltpu.VMEM((3, 4, 16, 32, N), f32),
                pltpu.VMEM((3, 4, 4, 32, N), f32), pltpu.VMEM((3, 2, 16, 32, N), f32), pltpu.VMEM((3, 15, 32, N), f32),
                pltpu.VMEM((1, N), f32), pltpu.VMEM((128, 1, N), f32), pltpu.VMEM((3, 2, 4, 16, 32, N), bf16),
            ] + [dma, dma((7,)), dma((3,))] + [dma] * 9 + [dma((3, 4)), dma((3, 4)), dma((3, 4)), dma((3, 2)), dma((3,)), dma, dma((3, 4)), dma((3, 4, 2)), dma((3, 4)), dma((3, 4, 4))]),
        compiler_params=pltpu.CompilerParams(vmem_limit_bytes=44 << 20, collective_id=0, has_side_effects=True),
        name="main",
    )(*(pltpu.with_memory_space_constraint(v, pltpu.HBM) for v in arrays))


def bwd_kernel(code, xs, dir_ref, out_ref, dir_out, ext, table, acc0, acc1, stage, sem):
    fill_tables(ext, table, True)
    zero = jnp.zeros((64, N), jnp.float32)

    @pl.loop(0, (E * C) // 64)
    def _(b):
        acc0[pl.ds(pl.multiple_of(b * 64, 64), 64), :] = zero
        acc1[pl.ds(pl.multiple_of(b * 64, 64), 64), :] = zero

    @pl.loop(0, T // BWD_UNROLL)
    def _(g):
        for u in range(BWD_UNROLL):
            for v, acc in ((0, acc0), (1, acc1)):
                w = code[v, g * BWD_UNROLL + u]
                block = w >> 16
                live = block < TILES
                x = xs[pl.ds(jnp.where(live, block, 0) * C, 16), :].astype(jnp.bfloat16)
                y = jnp.dot(x, table[w & 127], preferred_element_type=jnp.float32)
                r = jnp.where(live, (w >> 7) & 255, E) * C
                acc[pl.ds(r, 8), :] += y[:8]
                acc[pl.ds(r + 8, 4), :] += y[8:12]

    def leave(n):
        return pltpu.make_async_copy(stage.at[n], out_ref.at[n // 4, :, pl.ds(n % 4 * 64, 64)], sem.at[n])

    for n in range(8):
        acc = (acc0, acc1)[n // 4]

        @pl.loop(0, 8)
        def _(b):
            e0 = pl.multiple_of(b * 8, 8)
            for c in range(C):
                stage[n, c, pl.ds(e0, 8), :] = acc[pl.ds((n % 4 * 64 + e0) * C + c, 8, stride=C), :]

        leave(n).start()
    dir_out[...] = dir_ref[...]
    for n in range(8):
        leave(n).wait()


def backward(code, dirs, direction):
    f32 = jnp.float32
    return pl.pallas_call(
        bwd_kernel,
        out_shape=(jax.ShapeDtypeStruct((V, C, E, N), f32), jax.ShapeDtypeStruct((C, 1, 8, N), f32)),
        grid_spec=pltpu.PrefetchScalarGridSpec(
            num_scalar_prefetch=1, grid=(),
            in_specs=[pl.BlockSpec(memory_space=pltpu.VMEM)] * 2,
            out_specs=(pl.BlockSpec(memory_space=pl.ANY), pl.BlockSpec(memory_space=pltpu.VMEM)),
            scratch_shapes=[pltpu.VMEM((12, 136, N), f32), pltpu.VMEM((S, N, N), jnp.bfloat16),
                            pltpu.VMEM((E * C + 16, N), f32), pltpu.VMEM((E * C + 16, N), f32),
                            pltpu.VMEM((8, C, 64, N), f32), pltpu.SemaphoreType.DMA((8,))]),
        compiler_params=pltpu.CompilerParams(vmem_limit_bytes=44 << 20),
        name="bwd",
    )(code, dirs, direction)


def body(kernels, tile_owner, tile_source, tile_target, tile_seed, tile_count, prev_gradient, prev_step, precond):
    direction, dirs, code = main(tile_count.reshape(1, V), kernels, tile_owner.reshape(V, 1, T), tile_target, tile_seed, tile_source,
                                 prev_gradient, prev_step, precond)
    event_direction, direction = backward(code, dirs, direction)
    return direction, event_direction


def solution(mesh):
    in_specs = (
        P("ev", None, "mesh", None),
        P("ev", "mesh", None),
        P("ev", "mesh"),
        P("ev", "mesh"),
        P("ev", "mesh"),
        P("ev", "mesh"),
        P(None, "mesh", "ev", None),
        P(None, "mesh", "ev", None),
        P(None, "mesh", "ev", None),
    )
    out_specs = (P(None, "mesh", "ev", None), P("ev", None, "mesh", None))
    return jax.shard_map(body, mesh=mesh, in_specs=in_specs, out_specs=out_specs, check_vma=False)
```

```python
import jax
import jax.numpy as jnp
from jax import lax
from jax.experimental import pallas as pl
from jax.experimental.pallas import tpu as pltpu
from jax.sharding import PartitionSpec as P

C, N, E, T, V, S = 12, 128, 256, 512, 2, 84
TILES = V * T
AXES = ((0, 1, 2), (1, 2, 0), (2, 0, 1))
WEIGHT = (256, 64, 16)
HOPS = (0, 1, 2, 1)
MESH_ID = pl.DeviceIdType.MESH
FWD_UNROLL = 256
BWD_UNROLL = 128


def fill_tables(ext, table):
    i = lax.broadcasted_iota(jnp.int32, (136, N), 0).astype(jnp.float32) - 4.0
    j = lax.broadcasted_iota(jnp.int32, (136, N), 1).astype(jnp.float32)
    d = i - j
    for sp in range(3):
        spread = jnp.float32(0.55) + jnp.float32(0.1) * jnp.float32(sp)
        e = jnp.exp(-d * d / (jnp.float32(2.0) * spread * spread))
        for wt in range(4):
            weight = jnp.float32(0.1) + jnp.float32(0.1) * jnp.float32(wt)
            ext[wt * 3 + sp] = weight * e
    for k in range(12):
        for o in range(7):
            table[k * 7 + o] = ext[k, pl.ds(7 - o, N), :].astype(jnp.bfloat16)


def main_kernel(count_hbm, kern_hbm, owner_hbm, target_hbm, seed_hbm, source_hbm, pg_hbm, ps_hbm, pc_hbm, dir_ref, out_ref, code_ref, table,
                seed_s, source_s, count, owner, words, kern, fields, ext, xs, scr, con, give, take, own, s1, s2, pr, row, rows, tab,
                kern_sem, word_sem, field_sem, g_s, s1_s, s2_s, p_s, r_s, ap_s, ar_s, a2_s, ad_s,
                g_r, s1_r, s2_r, d2_r, p_r, r_r, ap_r, ar_r, a2_r, ad_r):
    e = lax.axis_index("ev")
    m = lax.axis_index("mesh")
    me = e * 16 + m
    at = (lax.rem(m, 4), lax.div(m, 4), lax.div(e, 2))
    core = lax.rem(e, 2)
    coord = [[a if o == 0 else lax.rem(a + o, 4) for o in range(4)] for a in at]

    ev_of = [(z * 2 + core, z * 2 + (1 - core)) for z in coord[2]]
    mesh_of = [[y * 4 + x for x in coord[0]] for y in coord[1]]

    def device(dx, dy, dz, other=False):
        return {"ev": ev_of[dz][int(other)], "mesh": mesh_of[dy][dx]}

    def place(k, r, i, j):
        off = [0, 0, 0]
        for axis, o in zip(AXES[k], (r, i, j)):
            off[axis] = o % 4
        return device(*off)

    partner = device(0, 0, 0, True)

    def copy(src, dst, ssem, rsem, where):
        return pltpu.make_async_remote_copy(src_ref=src, dst_ref=dst, send_sem=ssem, recv_sem=rsem,
                                            device_id=where, device_id_type=MESH_ID)

    def send(src, dst, ssem, rsem, where):
        copy(src, dst, ssem, rsem, where).start()

    def got(ref, ssem, rsem):
        copy(ref, ref, ssem, rsem, partner).wait_recv()

    def sent(ref, ssem, rsem):
        copy(ref, ref, ssem, rsem, partner).wait_send()

    load = pltpu.make_async_copy(kern_hbm, kern, kern_sem)
    load.start()
    indices = [pltpu.make_async_copy(src, dst, word_sem.at[n]) for n, (src, dst) in enumerate((
        (seed_hbm, seed_s), (source_hbm, source_s), (owner_hbm, owner), (target_hbm, words.at[0]), (seed_hbm, words.at[1]), (source_hbm, words.at[2]), (count_hbm, count)))]
    for one in indices:
        one.start()
    loads = [pltpu.make_async_copy(src, fields.at[n], field_sem.at[n]) for n, src in enumerate((pg_hbm, ps_hbm, pc_hbm))]
    for one in loads:
        one.start()
    barrier = pltpu.get_barrier_semaphore()

    everyone = [(dx, dy, dz, other) for dx in range(4) for dy in range(4) for dz in range(4) for other in (False, True)][1:]
    everyone.sort(key=lambda o: -(HOPS[o[0]] + HOPS[o[1]] + HOPS[o[2]]))
    for dx, dy, dz, other in everyone:
        pl.semaphore_signal(barrier, inc=1, device_id=device(dx, dy, dz, other), device_id_type=MESH_ID)

    fill_tables(ext, table)
    load.wait()
    for one in indices:
        one.wait()
    lanes = lax.broadcasted_iota(jnp.int32, (1, T), 1)
    blocks = []
    for v in range(V):
        home, goal = owner[v], words[0, v:v + 1, :]
        dx = ((home & 3) - at[0]) & 3
        dy = ((home >> 2) - at[1]) & 3
        dz = ((goal >> 4) - at[2]) & 3
        dc = ((goal >> 3) - core) & 1
        block = dx * 256 + dy * 64 + dz * 16 + dc * 8 + (goal & 7)
        block = jnp.where(lanes < count[0:1, v:v + 1], block, TILES)
        shape = words[1, v:v + 1, :]
        mirrored = 14 * ((shape * 37) >> 8) + 6 - shape
        code_ref[v:v + 1, :] = mirrored + (words[2, v:v + 1, :] << 7) + (block << 16)
        blocks.append(block)
    for v in range(V):
        @pl.loop(0, E // 16)
        def _(b):
            e0 = pl.multiple_of(b * 16, 16)
            for c in range(C):
                xs[pl.ds((v * E + e0) * C + c, 16, stride=C), :] = kern[v, c, pl.ds(e0, 16), :].astype(jnp.float32)

    @pl.loop(0, TILES // FWD_UNROLL)
    def _(g):
        t0 = g * FWD_UNROLL
        for u in range(FWD_UNROLL):
            t = (g % (T // FWD_UNROLL)) * FWD_UNROLL + u
            v = g // (T // FWD_UNROLL)
            x = xs[pl.ds((v * E + source_s[v, t]) * C, 16), :].astype(jnp.bfloat16)
            scr[u * 16:u * 16 + 16, :] = jnp.dot(x, table[seed_s[v, t]], preferred_element_type=jnp.float32)
        for h in range(FWD_UNROLL // 16):
            r0 = pl.multiple_of(t0 + h * 16, 16)
            for c in range(C):
                con[pl.ds(r0, 16), c * N:(c + 1) * N] = scr[pl.ds(h * 256 + c, 16, stride=16), :].astype(jnp.bfloat16)

    ids = lax.broadcasted_iota(jnp.int32, (128, N), 0)
    i_of, j_of, sub = ids >> 5, (ids >> 3) & 3, ids & 7
    block = jnp.concatenate(blocks, axis=1)
    pl.semaphore_wait(barrier, 127)

    def partial(k, r):
        a1, a2, a3 = AXES[k]
        rows_k = i_of * WEIGHT[a2] + j_of * WEIGHT[a3] + sub
        halves = []
        for core_offset in (8, 0):
            wanted = block - (r * WEIGHT[a1] + core_offset)
            halves.append(jnp.concatenate([(rows_k == wanted[:, l * N:(l + 1) * N]).astype(jnp.float32).astype(jnp.bfloat16) for l in range(8)], axis=1))
        total = jnp.dot(jnp.concatenate(halves, axis=0), con[:, k * 512:(k + 1) * 512], preferred_element_type=jnp.float32)
        for cc in range(4):
            give[k, r, :, cc * 8:cc * 8 + 8, :] = total[:128, cc * N:(cc + 1) * N].reshape(16, 8, N)
        send(give.at[k, r], take.at[k, r], g_s, g_r.at[k, r], partner)
        for cc in range(4):
            own[k, r, :, cc * 8:cc * 8 + 8, :] = total[128:, cc * N:(cc + 1) * N].reshape(16, 8, N)

    def straight(k, r, i):
        g, way = pl.ds(i * 4, 4), 0 if r == 1 else 1
        send(own.at[k, r, g], s2.at[k, way, g], s2_s, d2_r.at[k, i], place(k, r, 0, 0))

    def chip_sum(k, r):
        got(take.at[k, r], g_s, g_r.at[k, r])
        own[k, r] = own[k, r] + take[k, r]
        up, down = place(k, 1, 0, 0), place(k, 3, 0, 0)
        if r == 2:
            for i in (1, 2, 0, 3):
                send(own.at[k, 2, pl.ds(i * 4, 4)], s1.at[k, i], s1_s, s1_r.at[k, i], up if i < 2 else down)
        if r in (1, 3):
            straight(k, r, 2 if r == 1 else 1)

    steps = [(k, r) for r in (2, 1, 3, 0) for k in range(3)]
    lag = 3
    for n, (k, r) in enumerate(steps):
        partial(k, r)
        if n >= lag and steps[n - lag][1] != 0:
            chip_sum(*steps[n - lag])
    for i in (1, 2, 0, 3):
        g = pl.ds(i * 4, 4)
        for k in range(3):
            r, way = (1, 0) if i < 2 else (3, 1)
            got(s1.at[k, i], s1_s, s1_r.at[k, i])
            own[k, r, g] = own[k, r, g] + s1[k, i]
            send(own.at[k, r, g], s2.at[k, way, g], s2_s, s2_r.at[k, i], place(k, r, 0, 0))
            if i in (1, 2):
                straight(k, r, 0 if r == 3 else 3)
    for k in range(3):
        chip_sum(k, 0)
    far_first = sorted(range(1, 16), key=lambda q: -(HOPS[q // 4] + HOPS[q % 4]))
    for i in (1, 2, 0, 3):
        g = pl.ds(i * 4, 4)
        for k in range(3):
            got(s2.at[k, 1 if i < 2 else 0, g], s2_s, d2_r.at[k, i])
            got(s2.at[k, 0 if i < 2 else 1, g], s2_s, s2_r.at[k, i])
            own[k, 0, g] = own[k, 0, g] + s2[k, 0, g] + s2[k, 1, g]
            for q in far_first:
                if q // 4 == i:
                    send(own.at[k, 0, q], pr.at[k, q - 1], p_s, p_r.at[k], place(k, 0, i, q % 4))
    parts = []
    for k in range(3):
        got(pr.at[k], p_s, p_r.at[k])
        total = own[k, 0, 0]
        for q in range(15):
            total = total + pr[k, q]
        parts.append(total)
    gradient = jnp.concatenate(parts, axis=0)
    for one in loads:
        one.wait()
    prev_g, step, cond = (fields[n].reshape(96, N) for n in range(3))
    change = gradient - prev_g
    weighted = cond * change
    lane = lax.broadcasted_iota(jnp.int32, (1, N), 1)

    def summed(v):
        v = jnp.sum(v.reshape(12, 8, N), axis=0)
        return jnp.sum(jnp.sum(v, axis=0, keepdims=True), axis=1, keepdims=True)

    mine = jnp.zeros((1, N), jnp.float32)
    for n, v in enumerate((step * change, step * gradient, weighted * gradient, weighted * change)):
        mine = jnp.where(lane == n, summed(v), mine)
    row[...] = mine
    rows[me] = mine
    for dx, dy, dz, other in everyone:
        send(row, rows.at[me], r_s, r_r, device(dx, dy, dz, other))
    got(rows.at[pl.ds(0, 127)], r_s, r_r)
    totals = jnp.sum(rows[...], axis=0)
    curvature, slope, cross, self_ = (
        jnp.sum(jnp.where(lane == n, totals, 0.0), axis=1, keepdims=True) for n in range(4))
    alpha = slope / curvature
    beta = (cross - alpha * self_) / curvature
    scaled = cond * (gradient - alpha * change)
    direction = -(scaled + (alpha - beta) * step)
    rounded = direction.astype(jnp.bfloat16)
    for k in range(3):
        tab[k, 0, 0, 0] = rounded[k * 32:(k + 1) * 32]
    for q in far_first:
        i, j = q // 4, q % 4
        back = (-i % 4) * 4 + (-j % 4)
        for k in range(3):
            send(tab.at[k, 0, 0, 0], tab.at[k, 0, 0, back], ap_s, ap_r.at[k, back // 4], place(k, 0, i, j))

    dir_ref[...] = direction.reshape(12, 1, 8, N)
    out_ref[TILES * C:, :] = jnp.zeros((16, N), jnp.float32)

    def spread(k, rc, r, i):
        a1, a2, a3 = AXES[k]
        for j in range(4):
            base = r * WEIGHT[a1] + i * WEIGHT[a2] + j * WEIGHT[a3] + rc * 8
            piece = tab[k, rc, r, i * 4 + j].astype(jnp.float32)
            for cc in range(4):
                out_ref[pl.ds(base * C + k * 4 + cc, 8, stride=C), :] = piece[cc * 8:cc * 8 + 8]

    def across(k, r, i):
        g = pl.ds(i * 4, 4)
        send(tab.at[k, 0, r, g], tab.at[k, 1, r, g], ad_s, ad_r.at[k, r, i], partner)

    for i in (0, 1, 3, 2):
        g = pl.ds(i * 4, 4)
        for k in range(3):
            got(tab.at[k, 0, 0, pl.ds(1, 3) if i == 0 else g], ap_s, ap_r.at[k, i])
            send(tab.at[k, 0, 0, g], tab.at[k, 0, 2, g], a2_s, a2_r.at[k, i], place(k, 2, 0, 0))
            send(tab.at[k, 0, 0, g], tab.at[k, 0, 3, g], ar_s, ar_r.at[k, i, 0], place(k, 1, 0, 0))
            send(tab.at[k, 0, 0, g], tab.at[k, 0, 1, g], ar_s, ar_r.at[k, i, 1], place(k, 3, 0, 0))
            across(k, 0, i)
            spread(k, 0, 0, i)
    for i in (0, 1, 3, 2):
        g = pl.ds(i * 4, 4)
        for way, r in ((0, 3), (1, 1), (2, 2)):
            for k in range(3):
                got(tab.at[k, 0, r, g], ar_s, a2_r.at[k, i] if way == 2 else ar_r.at[k, i, way])
                across(k, r, i)
    for r in (0, 3, 1, 2):
        for i in (0, 1, 3, 2):
            for k in range(3):
                if r:
                    spread(k, 0, r, i)
    for r in (0, 3, 1, 2):
        for i in (0, 1, 3, 2):
            for k in range(3):
                got(tab.at[k, 1, r, pl.ds(i * 4, 4)], ad_s, ad_r.at[k, r, i])
                spread(k, 1, r, i)
    sent(give, g_s, g_r.at[0, 0])
    sent(s1, s1_s, s1_r.at[0, 0])
    sent(s2, s2_s, s2_r.at[0, 0])
    sent(pr, p_s, p_r.at[0])
    sent(rows.at[pl.ds(0, 127)], r_s, r_r)
    sent(tab.at[:, 0, 0, pl.ds(1, 15)], ap_s, ap_r.at[0, 0])
    sent(tab.at[:, 0, pl.ds(0, 2)], ar_s, ar_r.at[0, 0, 0])
    sent(tab.at[:, 0, 2], a2_s, a2_r.at[0, 0])
    sent(tab.at[:, 0], ad_s, ad_r.at[0, 0, 0])


def main(*arrays):
    dma = pltpu.SemaphoreType.DMA
    f32, bf16, i32 = jnp.float32, jnp.bfloat16, jnp.int32
    vmem = pl.BlockSpec(memory_space=pltpu.VMEM)
    return pl.pallas_call(
        main_kernel,
        out_shape=(jax.ShapeDtypeStruct((C, 1, 8, N), f32), jax.ShapeDtypeStruct((TILES * C + 16, N), f32), jax.ShapeDtypeStruct((V, T), i32),
                   jax.ShapeDtypeStruct((S, N, N), bf16)),
        grid_spec=pltpu.PrefetchScalarGridSpec(
            num_scalar_prefetch=0, grid=(),
            in_specs=[pl.BlockSpec(memory_space=pltpu.HBM)] * len(arrays),
            out_specs=(vmem, vmem, vmem, vmem),
            scratch_shapes=[
                pltpu.SMEM((V, T), i32), pltpu.SMEM((V, T), i32), pltpu.VMEM((1, V), i32), pltpu.VMEM((V, 1, T), i32), pltpu.VMEM((3, V, T), i32),
                pltpu.VMEM((V, C, E, N), bf16), pltpu.VMEM((3, C, 1, 8, N), f32), pltpu.VMEM((12, 136, N), f32),
                pltpu.VMEM((V * E * C + 16, N), f32), pltpu.VMEM((FWD_UNROLL * 16, N), f32), pltpu.VMEM((TILES, C * N), bf16),
                pltpu.VMEM((3, 4, 16, 32, N), f32), pltpu.VMEM((3, 4, 16, 32, N), f32), pltpu.VMEM((3, 4, 16, 32, N), f32),
                pltpu.VMEM((3, 4, 4, 32, N), f32), pltpu.VMEM((3, 2, 16, 32, N), f32), pltpu.VMEM((3, 15, 32, N), f32),
                pltpu.VMEM((1, N), f32), pltpu.VMEM((128, 1, N), f32), pltpu.VMEM((3, 2, 4, 16, 32, N), bf16),
            ] + [dma, dma((7,)), dma((3,))] + [dma] * 9 + [dma((3, 4)), dma((3, 4)), dma((3, 4)), dma((3, 4)), dma((3,)), dma, dma((3, 4)), dma((3, 4, 2)), dma((3, 4)), dma((3, 4, 4))]),
        compiler_params=pltpu.CompilerParams(vmem_limit_bytes=44 << 20, collective_id=0, has_side_effects=True),
        name="main",
    )(*(pltpu.with_memory_space_constraint(v, pltpu.HBM) for v in arrays))


def bwd_kernel(code, xs, table, dir_ref, out_ref, dir_out, acc0, acc1, stage, sem):
    zero = jnp.zeros((64, N), jnp.float32)

    @pl.loop(0, (E * C) // 64)
    def _(b):
        acc0[pl.ds(pl.multiple_of(b * 64, 64), 64), :] = zero
        acc1[pl.ds(pl.multiple_of(b * 64, 64), 64), :] = zero

    @pl.loop(0, T // BWD_UNROLL)
    def _(g):
        for u in range(BWD_UNROLL):
            for v, acc in ((0, acc0), (1, acc1)):
                w = code[v, g * BWD_UNROLL + u]
                block = w >> 16
                live = block < TILES
                x = xs[pl.ds(jnp.where(live, block, 0) * C, 16), :].astype(jnp.bfloat16)
                y = jnp.dot(x, table[w & 127], preferred_element_type=jnp.float32)
                r = jnp.where(live, (w >> 7) & 255, E) * C
                acc[pl.ds(r, 8), :] += y[:8]
                acc[pl.ds(r + 8, 4), :] += y[8:12]

    def leave(n):
        return pltpu.make_async_copy(stage.at[n], out_ref.at[n // 4, :, pl.ds(n % 4 * 64, 64)], sem.at[n])

    for n in range(8):
        acc = (acc0, acc1)[n // 4]

        @pl.loop(0, 8)
        def _(b):
            e0 = pl.multiple_of(b * 8, 8)
            for c in range(C):
                stage[n, c, pl.ds(e0, 8), :] = acc[pl.ds((n % 4 * 64 + e0) * C + c, 8, stride=C), :]

        leave(n).start()
    dir_out[...] = dir_ref[...]
    for n in range(8):
        leave(n).wait()


def backward(code, dirs, table, direction):
    f32 = jnp.float32
    return pl.pallas_call(
        bwd_kernel,
        out_shape=(jax.ShapeDtypeStruct((V, C, E, N), f32), jax.ShapeDtypeStruct((C, 1, 8, N), f32)),
        grid_spec=pltpu.PrefetchScalarGridSpec(
            num_scalar_prefetch=1, grid=(),
            in_specs=[pl.BlockSpec(memory_space=pltpu.VMEM)] * 3,
            out_specs=(pl.BlockSpec(memory_space=pl.ANY), pl.BlockSpec(memory_space=pltpu.VMEM)),
            scratch_shapes=[pltpu.VMEM((E * C + 16, N), f32), pltpu.VMEM((E * C + 16, N), f32),
                            pltpu.VMEM((8, C, 64, N), f32), pltpu.SemaphoreType.DMA((8,))]),
        compiler_params=pltpu.CompilerParams(vmem_limit_bytes=44 << 20),
        name="bwd",
    )(code, dirs, table, direction)


def body(kernels, tile_owner, tile_source, tile_target, tile_seed, tile_count, prev_gradient, prev_step, precond):
    direction, dirs, code, table = main(tile_count.reshape(1, V), kernels, tile_owner.reshape(V, 1, T), tile_target, tile_seed, tile_source,
                                 prev_gradient, prev_step, precond)
    event_direction, direction = backward(code, dirs, table, direction)
    return direction, event_direction


def solution(mesh):
    in_specs = (
        P("ev", None, "mesh", None),
        P("ev", "mesh", None),
        P("ev", "mesh"),
        P("ev", "mesh"),
        P("ev", "mesh"),
        P("ev", "mesh"),
        P(None, "mesh", "ev", None),
        P(None, "mesh", "ev", None),
        P(None, "mesh", "ev", None),
    )
    out_specs = (P(None, "mesh", "ev", None), P("ev", None, "mesh", None))
    return jax.shard_map(body, mesh=mesh, in_specs=in_specs, out_specs=out_specs, check_vma=False)
```

```python
import jax
import jax.numpy as jnp
from jax import lax
from jax.experimental import pallas as pl
from jax.experimental.pallas import tpu as pltpu
from jax.sharding import PartitionSpec as P

C, N, E, T, V, S = 12, 128, 256, 512, 2, 84
TILES = V * T
AXES = ((0, 1, 2), (1, 2, 0), (2, 0, 1))
WEIGHT = (256, 64, 16)
HOPS = (0, 1, 2, 1)
MESH_ID = pl.DeviceIdType.MESH
FWD_UNROLL = 256
BWD_UNROLL = 128


def fill_tables(ext, table):
    i = lax.broadcasted_iota(jnp.int32, (136, N), 0).astype(jnp.float32) - 4.0
    j = lax.broadcasted_iota(jnp.int32, (136, N), 1).astype(jnp.float32)
    d = i - j
    for sp in range(3):
        spread = jnp.float32(0.55) + jnp.float32(0.1) * jnp.float32(sp)
        e = jnp.exp(-d * d / (jnp.float32(2.0) * spread * spread))
        for wt in range(4):
            weight = jnp.float32(0.1) + jnp.float32(0.1) * jnp.float32(wt)
            ext[wt * 3 + sp] = weight * e
    for k in range(12):
        for o in range(7):
            table[k * 7 + o] = ext[k, pl.ds(7 - o, N), :].astype(jnp.bfloat16)


def main_kernel(count_hbm, kern_hbm, owner_hbm, target_hbm, seed_hbm, source_hbm, pg_hbm, ps_hbm, pc_hbm, dir_ref, out_ref, code_ref, table,
                seed_s, source_s, count, owner, words, kern, fields, ext, xs, scr, con, give, take, own, s1, s2, pr, row, rows, tab,
                kern_sem, word_sem, field_sem, g_s, s1_s, s2_s, p_s, r_s, ap_s, ar_s, a2_s, ad_s,
                g_r, s1_r, s2_r, d2_r, p_r, r_r, ap_r, ar_r, a2_r, ad_r):
    e = lax.axis_index("ev")
    m = lax.axis_index("mesh")
    me = e * 16 + m
    at = (lax.rem(m, 4), lax.div(m, 4), lax.div(e, 2))
    core = lax.rem(e, 2)
    coord = [[a if o == 0 else lax.rem(a + o, 4) for o in range(4)] for a in at]

    ev_of = [(z * 2 + core, z * 2 + (1 - core)) for z in coord[2]]
    mesh_of = [[y * 4 + x for x in coord[0]] for y in coord[1]]

    def device(dx, dy, dz, other=False):
        return {"ev": ev_of[dz][int(other)], "mesh": mesh_of[dy][dx]}

    def place(k, r, i, j):
        off = [0, 0, 0]
        for axis, o in zip(AXES[k], (r, i, j)):
            off[axis] = o % 4
        return device(*off)

    partner = device(0, 0, 0, True)

    def copy(src, dst, ssem, rsem, where):
        return pltpu.make_async_remote_copy(src_ref=src, dst_ref=dst, send_sem=ssem, recv_sem=rsem,
                                            device_id=where, device_id_type=MESH_ID)

    def send(src, dst, ssem, rsem, where):
        copy(src, dst, ssem, rsem, where).start()

    def got(ref, ssem, rsem):
        copy(ref, ref, ssem, rsem, partner).wait_recv()

    def sent(ref, ssem, rsem):
        copy(ref, ref, ssem, rsem, partner).wait_send()

    load = pltpu.make_async_copy(kern_hbm, kern, kern_sem)
    load.start()
    indices = [pltpu.make_async_copy(src, dst, word_sem.at[n]) for n, (src, dst) in enumerate((
        (seed_hbm, seed_s), (source_hbm, source_s), (owner_hbm, owner), (target_hbm, words.at[0]), (seed_hbm, words.at[1]), (source_hbm, words.at[2]), (count_hbm, count)))]
    for one in indices:
        one.start()
    loads = [pltpu.make_async_copy(src, fields.at[n], field_sem.at[n]) for n, src in enumerate((pg_hbm, ps_hbm, pc_hbm))]
    for one in loads:
        one.start()
    barrier = pltpu.get_barrier_semaphore()

    everyone = [(dx, dy, dz, other) for dx in range(4) for dy in range(4) for dz in range(4) for other in (False, True)][1:]
    everyone.sort(key=lambda o: -(HOPS[o[0]] + HOPS[o[1]] + HOPS[o[2]]))
    for dx, dy, dz, other in everyone:
        pl.semaphore_signal(barrier, inc=1, device_id=device(dx, dy, dz, other), device_id_type=MESH_ID)

    fill_tables(ext, table)
    load.wait()
    for one in indices:
        one.wait()
    lanes = lax.broadcasted_iota(jnp.int32, (1, T), 1)
    blocks = []
    for v in range(V):
        home, goal = owner[v], words[0, v:v + 1, :]
        dx = ((home & 3) - at[0]) & 3
        dy = ((home >> 2) - at[1]) & 3
        dz = ((goal >> 4) - at[2]) & 3
        dc = ((goal >> 3) - core) & 1
        block = dx * 256 + dy * 64 + dz * 16 + dc * 8 + (goal & 7)
        block = jnp.where(lanes < count[0:1, v:v + 1], block, TILES)
        shape = words[1, v:v + 1, :]
        mirrored = 14 * ((shape * 37) >> 8) + 6 - shape
        code_ref[v:v + 1, :] = mirrored + (words[2, v:v + 1, :] << 7) + (block << 16)
        blocks.append(block)
    for v in range(V):
        @pl.loop(0, E // 16)
        def _(b):
            e0 = pl.multiple_of(b * 16, 16)
            for c in range(C):
                xs[pl.ds((v * E + e0) * C + c, 16, stride=C), :] = kern[v, c, pl.ds(e0, 16), :].astype(jnp.float32)

    @pl.loop(0, TILES // FWD_UNROLL)
    def _(g):
        t0 = g * FWD_UNROLL
        for u in range(FWD_UNROLL):
            t = (g % (T // FWD_UNROLL)) * FWD_UNROLL + u
            v = g // (T // FWD_UNROLL)
            x = xs[pl.ds((v * E + source_s[v, t]) * C, 16), :].astype(jnp.bfloat16)
            scr[u * 16:u * 16 + 16, :] = jnp.dot(x, table[seed_s[v, t]], preferred_element_type=jnp.float32)
        for h in range(FWD_UNROLL // 16):
            r0 = pl.multiple_of(t0 + h * 16, 16)
            for c in range(C):
                con[pl.ds(r0, 16), c * N:(c + 1) * N] = scr[pl.ds(h * 256 + c, 16, stride=16), :].astype(jnp.bfloat16)

    ids = lax.broadcasted_iota(jnp.int32, (128, N), 0)
    i_of, j_of, sub = ids >> 5, (ids >> 3) & 3, ids & 7
    block = jnp.concatenate(blocks, axis=1)
    pl.semaphore_wait(barrier, 127)

    def partial(k, r):
        a1, a2, a3 = AXES[k]
        rows_k = i_of * WEIGHT[a2] + j_of * WEIGHT[a3] + sub
        halves = []
        for core_offset in (8, 0):
            wanted = block - (r * WEIGHT[a1] + core_offset)
            halves.append(jnp.concatenate([(rows_k == wanted[:, l * N:(l + 1) * N]).astype(jnp.float32).astype(jnp.bfloat16) for l in range(8)], axis=1))
        total = jnp.dot(jnp.concatenate(halves, axis=0), con[:, k * 512:(k + 1) * 512], preferred_element_type=jnp.float32)
        for cc in range(4):
            give[k, r, :, cc * 8:cc * 8 + 8, :] = total[:128, cc * N:(cc + 1) * N].reshape(16, 8, N)
        send(give.at[k, r], take.at[k, r], g_s, g_r.at[k, r], partner)
        for cc in range(4):
            own[k, r, :, cc * 8:cc * 8 + 8, :] = total[128:, cc * N:(cc + 1) * N].reshape(16, 8, N)

    def chip_sum(k, r):
        got(take.at[k, r], g_s, g_r.at[k, r])
        own[k, r] = own[k, r] + take[k, r]
        up, down = place(k, 1, 0, 0), place(k, 3, 0, 0)
        if r == 2:
            for i in (1, 2, 0, 3):
                send(own.at[k, 2, pl.ds(i * 4, 4)], s1.at[k, i], s1_s, s1_r.at[k, i], up if i < 2 else down)
        if r == 1:
            send(own.at[k, 1, pl.ds(8, 8)], s2.at[k, 0, pl.ds(8, 8)], s2_s, d2_r.at[k, 0], up)
        if r == 3:
            send(own.at[k, 3, pl.ds(0, 8)], s2.at[k, 1, pl.ds(0, 8)], s2_s, d2_r.at[k, 1], down)

    steps = [(k, r) for r in (2, 1, 3, 0) for k in range(3)]
    lag = 2
    for n, (k, r) in enumerate(steps):
        partial(k, r)
        if n >= lag:
            chip_sum(*steps[n - lag])
    for k, r in steps[len(steps) - lag:]:
        chip_sum(k, r)
    for i in (1, 2, 0, 3):
        g = pl.ds(i * 4, 4)
        for k in range(3):
            r, way = (1, 0) if i < 2 else (3, 1)
            got(s1.at[k, i], s1_s, s1_r.at[k, i])
            own[k, r, g] = own[k, r, g] + s1[k, i]
            send(own.at[k, r, g], s2.at[k, way, g], s2_s, s2_r.at[k, i], place(k, r, 0, 0))
    far_first = sorted(range(1, 16), key=lambda q: -(HOPS[q // 4] + HOPS[q % 4]))
    for i in (1, 2, 0, 3):
        g = pl.ds(i * 4, 4)
        for k in range(3):
            if i == 1:
                got(s2.at[k, 0, pl.ds(8, 8)], s2_s, d2_r.at[k, 0])
                got(s2.at[k, 1, pl.ds(0, 8)], s2_s, d2_r.at[k, 1])
            got(s2.at[k, 0 if i < 2 else 1, g], s2_s, s2_r.at[k, i])
            own[k, 0, g] = own[k, 0, g] + s2[k, 0, g] + s2[k, 1, g]
            for q in far_first:
                if q // 4 == i:
                    send(own.at[k, 0, q], pr.at[k, q - 1], p_s, p_r.at[k], place(k, 0, i, q % 4))
    parts = []
    for k in range(3):
        got(pr.at[k], p_s, p_r.at[k])
        total = own[k, 0, 0]
        for q in range(15):
            total = total + pr[k, q]
        parts.append(total)
    gradient = jnp.concatenate(parts, axis=0)
    for one in loads:
        one.wait()
    prev_g, step, cond = (fields[n].reshape(96, N) for n in range(3))
    change = gradient - prev_g
    weighted = cond * change
    lane = lax.broadcasted_iota(jnp.int32, (1, N), 1)

    def summed(v):
        v = jnp.sum(v.reshape(12, 8, N), axis=0)
        return jnp.sum(jnp.sum(v, axis=0, keepdims=True), axis=1, keepdims=True)

    mine = jnp.zeros((1, N), jnp.float32)
    for n, v in enumerate((step * change, step * gradient, weighted * gradient, weighted * change)):
        mine = jnp.where(lane == n, summed(v), mine)
    row[...] = mine
    rows[me] = mine
    for dx, dy, dz, other in everyone:
        send(row, rows.at[me], r_s, r_r, device(dx, dy, dz, other))
    got(rows.at[pl.ds(0, 127)], r_s, r_r)
    totals = jnp.sum(rows[...], axis=0)
    curvature, slope, cross, self_ = (
        jnp.sum(jnp.where(lane == n, totals, 0.0), axis=1, keepdims=True) for n in range(4))
    alpha = slope / curvature
    beta = (cross - alpha * self_) / curvature
    scaled = cond * (gradient - alpha * change)
    direction = -(scaled + (alpha - beta) * step)
    rounded = direction.astype(jnp.bfloat16)
    for k in range(3):
        tab[k, 0, 0, 0] = rounded[k * 32:(k + 1) * 32]
    for q in far_first:
        i, j = q // 4, q % 4
        back = (-i % 4) * 4 + (-j % 4)
        for k in range(3):
            send(tab.at[k, 0, 0, 0], tab.at[k, 0, 0, back], ap_s, ap_r.at[k, back // 4], place(k, 0, i, j))

    dir_ref[...] = direction.reshape(12, 1, 8, N)
    out_ref[TILES * C:, :] = jnp.zeros((16, N), jnp.float32)

    def spread(k, rc, r, i):
        a1, a2, a3 = AXES[k]
        for j in range(4):
            base = r * WEIGHT[a1] + i * WEIGHT[a2] + j * WEIGHT[a3] + rc * 8
            piece = tab[k, rc, r, i * 4 + j].astype(jnp.float32)
            for cc in range(4):
                out_ref[pl.ds(base * C + k * 4 + cc, 8, stride=C), :] = piece[cc * 8:cc * 8 + 8]

    def across(k, r, i):
        g = pl.ds(i * 4, 4)
        send(tab.at[k, 0, r, g], tab.at[k, 1, r, g], ad_s, ad_r.at[k, r, i], partner)

    for i in (0, 1, 3, 2):
        g = pl.ds(i * 4, 4)
        for k in range(3):
            got(tab.at[k, 0, 0, pl.ds(1, 3) if i == 0 else g], ap_s, ap_r.at[k, i])
            send(tab.at[k, 0, 0, g], tab.at[k, 0, 2, g], a2_s, a2_r.at[k, i], place(k, 2, 0, 0))
            send(tab.at[k, 0, 0, g], tab.at[k, 0, 3, g], ar_s, ar_r.at[k, i, 0], place(k, 1, 0, 0))
            send(tab.at[k, 0, 0, g], tab.at[k, 0, 1, g], ar_s, ar_r.at[k, i, 1], place(k, 3, 0, 0))
            across(k, 0, i)
            spread(k, 0, 0, i)
    for i in (0, 1, 3, 2):
        g = pl.ds(i * 4, 4)
        for way, r in ((0, 3), (1, 1), (2, 2)):
            for k in range(3):
                got(tab.at[k, 0, r, g], ar_s, a2_r.at[k, i] if way == 2 else ar_r.at[k, i, way])
                across(k, r, i)
    for r in (0, 3, 1, 2):
        for i in (0, 1, 3, 2):
            for k in range(3):
                if r:
                    spread(k, 0, r, i)
    for r in (0, 3, 1, 2):
        for i in (0, 1, 3, 2):
            for k in range(3):
                got(tab.at[k, 1, r, pl.ds(i * 4, 4)], ad_s, ad_r.at[k, r, i])
                spread(k, 1, r, i)
    sent(give, g_s, g_r.at[0, 0])
    sent(s1, s1_s, s1_r.at[0, 0])
    sent(s2, s2_s, s2_r.at[0, 0])
    sent(pr, p_s, p_r.at[0])
    sent(rows.at[pl.ds(0, 127)], r_s, r_r)
    sent(tab.at[:, 0, 0, pl.ds(1, 15)], ap_s, ap_r.at[0, 0])
    sent(tab.at[:, 0, pl.ds(0, 2)], ar_s, ar_r.at[0, 0, 0])
    sent(tab.at[:, 0, 2], a2_s, a2_r.at[0, 0])
    sent(tab.at[:, 0], ad_s, ad_r.at[0, 0, 0])


def main(*arrays):
    dma = pltpu.SemaphoreType.DMA
    f32, bf16, i32 = jnp.float32, jnp.bfloat16, jnp.int32
    vmem = pl.BlockSpec(memory_space=pltpu.VMEM)
    return pl.pallas_call(
        main_kernel,
        out_shape=(jax.ShapeDtypeStruct((C, 1, 8, N), f32), jax.ShapeDtypeStruct((TILES * C + 16, N), f32), jax.ShapeDtypeStruct((V, T), i32),
                   jax.ShapeDtypeStruct((S, N, N), bf16)),
        grid_spec=pltpu.PrefetchScalarGridSpec(
            num_scalar_prefetch=0, grid=(),
            in_specs=[pl.BlockSpec(memory_space=pltpu.HBM)] * len(arrays),
            out_specs=(vmem, vmem, vmem, vmem),
            scratch_shapes=[
                pltpu.SMEM((V, T), i32), pltpu.SMEM((V, T), i32), pltpu.VMEM((1, V), i32), pltpu.VMEM((V, 1, T), i32), pltpu.VMEM((3, V, T), i32),
                pltpu.VMEM((V, C, E, N), bf16), pltpu.VMEM((3, C, 1, 8, N), f32), pltpu.VMEM((12, 136, N), f32),
                pltpu.VMEM((V * E * C + 16, N), f32), pltpu.VMEM((FWD_UNROLL * 16, N), f32), pltpu.VMEM((TILES, C * N), bf16),
                pltpu.VMEM((3, 4, 16, 32, N), f32), pltpu.VMEM((3, 4, 16, 32, N), f32), pltpu.VMEM((3, 4, 16, 32, N), f32),
                pltpu.VMEM((3, 4, 4, 32, N), f32), pltpu.VMEM((3, 2, 16, 32, N), f32), pltpu.VMEM((3, 15, 32, N), f32),
                pltpu.VMEM((1, N), f32), pltpu.VMEM((128, 1, N), f32), pltpu.VMEM((3, 2, 4, 16, 32, N), bf16),
            ] + [dma, dma((7,)), dma((3,))] + [dma] * 9 + [dma((3, 4)), dma((3, 4)), dma((3, 4)), dma((3, 2)), dma((3,)), dma, dma((3, 4)), dma((3, 4, 2)), dma((3, 4)), dma((3, 4, 4))]),
        compiler_params=pltpu.CompilerParams(vmem_limit_bytes=44 << 20, collective_id=0, has_side_effects=True),
        name="main",
    )(*(pltpu.with_memory_space_constraint(v, pltpu.HBM) for v in arrays))


def bwd_kernel(code, xs, table, dir_ref, out_ref, dir_out, acc0, acc1, stage, sem):
    zero = jnp.zeros((64, N), jnp.float32)

    @pl.loop(0, (E * C) // 64)
    def _(b):
        acc0[pl.ds(pl.multiple_of(b * 64, 64), 64), :] = zero
        acc1[pl.ds(pl.multiple_of(b * 64, 64), 64), :] = zero

    @pl.loop(0, T // BWD_UNROLL)
    def _(g):
        for u in range(BWD_UNROLL):
            for v, acc in ((0, acc0), (1, acc1)):
                w = code[v, g * BWD_UNROLL + u]
                block = w >> 16
                live = block < TILES
                x = xs[pl.ds(jnp.where(live, block, 0) * C, 16), :].astype(jnp.bfloat16)
                y = jnp.dot(x, table[w & 127], preferred_element_type=jnp.float32)
                r = jnp.where(live, (w >> 7) & 255, E) * C
                acc[pl.ds(r, 8), :] += y[:8]
                acc[pl.ds(r + 8, 4), :] += y[8:12]

    def leave(n):
        return pltpu.make_async_copy(stage.at[n], out_ref.at[n // 4, :, pl.ds(n % 4 * 64, 64)], sem.at[n])

    for n in range(8):
        acc = (acc0, acc1)[n // 4]

        @pl.loop(0, 8)
        def _(b):
            e0 = pl.multiple_of(b * 8, 8)
            for c in range(C):
                stage[n, c, pl.ds(e0, 8), :] = acc[pl.ds((n % 4 * 64 + e0) * C + c, 8, stride=C), :]

        leave(n).start()
    dir_out[...] = dir_ref[...]
    for n in range(8):
        leave(n).wait()


def backward(code, dirs, table, direction):
    f32 = jnp.float32
    return pl.pallas_call(
        bwd_kernel,
        out_shape=(jax.ShapeDtypeStruct((V, C, E, N), f32), jax.ShapeDtypeStruct((C, 1, 8, N), f32)),
        grid_spec=pltpu.PrefetchScalarGridSpec(
            num_scalar_prefetch=1, grid=(),
            in_specs=[pl.BlockSpec(memory_space=pltpu.VMEM)] * 3,
            out_specs=(pl.BlockSpec(memory_space=pl.ANY), pl.BlockSpec(memory_space=pltpu.VMEM)),
            scratch_shapes=[pltpu.VMEM((E * C + 16, N), f32), pltpu.VMEM((E * C + 16, N), f32),
                            pltpu.VMEM((8, C, 64, N), f32), pltpu.SemaphoreType.DMA((8,))]),
        compiler_params=pltpu.CompilerParams(vmem_limit_bytes=44 << 20),
        name="bwd",
    )(code, dirs, table, direction)


def body(kernels, tile_owner, tile_source, tile_target, tile_seed, tile_count, prev_gradient, prev_step, precond):
    direction, dirs, code, table = main(tile_count.reshape(1, V), kernels, tile_owner.reshape(V, 1, T), tile_target, tile_seed, tile_source,
                                 prev_gradient, prev_step, precond)
    event_direction, direction = backward(code, dirs, table, direction)
    return direction, event_direction


def solution(mesh):
    in_specs = (
        P("ev", None, "mesh", None),
        P("ev", "mesh", None),
        P("ev", "mesh"),
        P("ev", "mesh"),
        P("ev", "mesh"),
        P("ev", "mesh"),
        P(None, "mesh", "ev", None),
        P(None, "mesh", "ev", None),
        P(None, "mesh", "ev", None),
    )
    out_specs = (P(None, "mesh", "ev", None), P("ev", None, "mesh", None))
    return jax.shard_map(body, mesh=mesh, in_specs=in_specs, out_specs=out_specs, check_vma=False)
```
